32 devices in a mesh: grp: 4 (over z), tp: 4 (over y, x), rep: 2 (over core).
Axes of the slice: x: 2, y: 2, z: 4, core: 2. Of those that a mesh axis runs over, the one named last changes fastest.
Arguments:
- query_rows: bfloat16 [4, 1024, 2048], P('tp', ('grp', 'rep')), may hold values from -120 to 120
- key_rows: bfloat16 [4, 1024, 512], P('tp', ('grp', 'rep')), may hold values from -6 to 6, as said below
- value_rows: bfloat16 [4, 1024, 512], P('tp', ('grp', 'rep')), may hold values from -6 to 6
- teacher_codes: bfloat16 [4, 1024, 4096], P(None, ('grp', 'rep'), 'tp'), may hold values from -6 to 6
- teacher_scales: bfloat16 [4, 1024, 32], P(None, ('grp', 'rep'), 'tp'), may hold values from 0.099609375 to 1
- projection: bfloat16 [2048, 4096], P(None, ('grp', 'rep')), may hold values from -0.125 to 0.125
Outputs:
- grad_query: bfloat16 [4, 1024, 2048], P('tp', ('grp', 'rep'))
- grad_key: bfloat16 [4, 1024, 512], P('tp', ('grp', 'rep'))
- grad_value: bfloat16 [4, 1024, 512], P('tp', ('grp', 'rep'))
The draws below stay inside these ranges and needn't reach their ends.
Inputs may be any that keep to these rules, and one draw needn't show every extreme that they name: `key_rows`: keys of every head.
All inputs are finite; a program needn't handle non-finite values.
Results may differ from the reference program's by a relative error of at most 0.014.
Values may be sent and summed in bfloat16 or wider, within the bound.
A program may use at most 128 MiB of HBM per device.

```python
import math
import jax
import jax.numpy as jnp
from jax import lax

TOK_DEV = 128
HEADS = 16
KV_HEADS = 4
HEAD_DIM = 128
COLS = 4096
QBLOCK = 128
SEQS = 4
SEQ_LEN = 1024
N_GRP = 4
N_REP = 2


def paired_fields(key):
    query_noise = jax.random.normal(jax.random.fold_in(key, 101), (SEQS, SEQ_LEN, HEADS, HEAD_DIM), jnp.float32)
    key_noise = jax.random.normal(jax.random.fold_in(key, 202), (SEQS, SEQ_LEN, KV_HEADS, HEAD_DIM), jnp.float32)
    keys_field = jnp.clip(key_noise, -6.0, 6.0)
    queries_field = jnp.clip(2.0 * query_noise, -12.0, 12.0)
    queries_field = queries_field.reshape(SEQS, SEQ_LEN, HEADS * HEAD_DIM)
    keys_field = keys_field.reshape(SEQS, SEQ_LEN, KV_HEADS * HEAD_DIM)
    return (queries_field, keys_field)


def draw_query_rows(key, part):
    return paired_fields(key)[0].astype(jnp.bfloat16)


def draw_key_rows(key, part):
    return paired_fields(key)[1].astype(jnp.bfloat16)


def block_levels(stream_key, dims, shards, least, top_value):
    gain, own = 1.0, jax.random.fold_in(stream_key, 6)
    for axis_at, parts in shards:
        draws = jnp.exp(jax.random.uniform(jax.random.fold_in(own, axis_at), (parts,), jnp.float32, least / len(shards), top_value / len(shards)))
        gain = gain * jnp.repeat(draws, dims[axis_at] // parts).reshape([-1 if axis == axis_at else 1 for axis in range(len(dims))])
    return gain


def bell_draw(own_key, dims, width, reach, shards=(), kind=jnp.bfloat16):
    array = width * jax.random.normal(own_key, dims, jnp.float32)
    if shards:
        array = array * block_levels(own_key, dims, shards, -0.22, 0.18)
    return jnp.clip(array, -reach, reach).astype(kind)


def setup_inputs(seed: int = 0) -> dict:
    splits = jax.random.split(jax.random.key(seed), 7)
    return {
        "query_rows": draw_query_rows(jax.random.fold_in(splits[6], 71), 0),
        "key_rows": draw_key_rows(jax.random.fold_in(splits[6], 71), 0),
        "value_rows": bell_draw(splits[2], (SEQS, SEQ_LEN, KV_HEADS * HEAD_DIM), 1.0, 6.0, ((0, 4), (1, 8))),
        "teacher_codes": bell_draw(splits[3], (SEQS, SEQ_LEN, COLS), 1.0, 6.0, ((1, 8), (2, 4))),
        "teacher_scales": jnp.clip(jnp.exp(math.log(1.0) - 2.306499 * jax.random.uniform(splits[4], (SEQS, SEQ_LEN, COLS // QBLOCK), jnp.float32) ** block_levels(splits[4], (SEQS, SEQ_LEN, COLS // QBLOCK), ((1, 8), (2, 4)), -0.2, 0.2)), 0.099609375, 1.0).astype(jnp.bfloat16),
        "projection": bell_draw(splits[5], (HEADS * HEAD_DIM, COLS), (HEADS * HEAD_DIM) ** -0.5, 0.125, ((1, 8),)),
    }


masked_low = -1e+30

def reference(query_rows, key_rows, value_rows, teacher_codes, teacher_scales, projection):
    group_size = HEADS // KV_HEADS
    part_count = N_GRP * N_REP
    col_width = COLS // part_count
    block_count = SEQ_LEN // TOK_DEV
    inv_root = 1.0 / math.sqrt(HEAD_DIM)
    row_ids = jnp.arange(TOK_DEV, dtype=jnp.int32)
    col_ids = jnp.arange(SEQ_LEN, dtype=jnp.int32)
    highest = lax.Precision.HIGHEST

    def one_slab(slab_data):
        slab_query, slab_key, slab_value, slab_codes, slab_scales = slab_data
        key_heads = slab_key.reshape(SEQ_LEN, KV_HEADS, HEAD_DIM).transpose(1, 0, 2).astype(jnp.float32)
        value_heads = slab_value.reshape(SEQ_LEN, KV_HEADS, HEAD_DIM).transpose(1, 0, 2).astype(jnp.float32)

        def scan_step(running, block_index):
            grad_keys, grad_values = running
            first = (block_index * TOK_DEV).astype(jnp.int32)
            query_part = lax.dynamic_slice_in_dim(slab_query, first, TOK_DEV, 0)
            queries = query_part.reshape(TOK_DEV, KV_HEADS, group_size, HEAD_DIM).transpose(1, 2, 0, 3).astype(jnp.float32)
            raw_scores = jnp.einsum('hgqd,hkd->hgqk', queries, key_heads, precision=highest) * inv_root
            allowed = col_ids[None, :] <= (first + row_ids)[:, None]
            scores = jnp.where(allowed, raw_scores, masked_low)
            row_peak = scores.max(-1)
            shifted = jnp.exp(scores - row_peak[..., None])
            row_total = shifted.sum(-1)
            probs = shifted / row_total[..., None]
            prob_low = probs.astype(jnp.bfloat16)
            attn_wide = jnp.einsum('hgqk,hkd->hgqd', prob_low.astype(jnp.float32), value_heads, precision=highest)
            attn_flat = attn_wide.transpose(2, 0, 1, 3).reshape(TOK_DEV, HEADS * HEAD_DIM)
            attn_low = attn_flat.astype(jnp.bfloat16)
            approx = jnp.dot(attn_low, projection, preferred_element_type=jnp.float32)
            code_rows = lax.dynamic_slice_in_dim(slab_codes, first, TOK_DEV, 0).astype(jnp.float32)
            scale_rows = lax.dynamic_slice_in_dim(slab_scales, first, TOK_DEV, 0).astype(jnp.float32)
            target = (code_rows.reshape(TOK_DEV, COLS // QBLOCK, QBLOCK) * scale_rows[..., None]).reshape(TOK_DEV, COLS)
            errors = (approx - target).astype(jnp.bfloat16)
            grad_attn = jnp.zeros((TOK_DEV, HEADS * HEAD_DIM), jnp.float32)
            for column_block in range(part_count):
                lower = column_block * col_width
                term = jnp.dot(errors[:, lower:lower + col_width], projection[:, lower:lower + col_width].T, preferred_element_type=jnp.float32)
                term_low = lax.optimization_barrier(term.astype(jnp.bfloat16))
                grad_attn = grad_attn + term_low.astype(jnp.float32)
            grad_low = grad_attn.astype(jnp.bfloat16)
            grad_heads = grad_low.reshape(TOK_DEV, KV_HEADS, group_size, HEAD_DIM).transpose(1, 2, 0, 3).astype(jnp.float32)
            row_delta = (grad_heads * attn_wide).sum(-1)
            grad_prob = jnp.einsum('hgqd,hkd->hgqk', grad_heads, value_heads, precision=highest)
            grad_score = (probs * (grad_prob - row_delta[..., None]) * inv_root).astype(jnp.bfloat16).astype(jnp.float32)
            grad_queries = jnp.einsum('hgqk,hkd->hgqd', grad_score, key_heads, precision=highest)
            grad_queries = grad_queries.transpose(2, 0, 1, 3).reshape(TOK_DEV, HEADS * HEAD_DIM).astype(jnp.bfloat16)
            key_piece = jnp.einsum('hgqk,hgqd->hkd', grad_score, queries, precision=highest)
            value_piece = jnp.einsum('hgqk,hgqd->hkd', prob_low.astype(jnp.float32), grad_heads, precision=highest)
            key_low = lax.optimization_barrier(key_piece.astype(jnp.bfloat16))
            value_low = lax.optimization_barrier(value_piece.astype(jnp.bfloat16))
            grad_keys = grad_keys + key_low.astype(jnp.float32)
            grad_values = grad_values + value_low.astype(jnp.float32)
            return ((grad_keys, grad_values), grad_queries)
        zeros_kv = jnp.zeros((KV_HEADS, SEQ_LEN, HEAD_DIM), jnp.float32)
        (grad_keys, grad_values), grad_queries = lax.scan(scan_step, (zeros_kv, zeros_kv), jnp.arange(block_count, dtype=jnp.int32))
        grad_queries = grad_queries.reshape(SEQ_LEN, HEADS * HEAD_DIM)
        grad_keys = grad_keys.transpose(1, 0, 2).reshape(SEQ_LEN, KV_HEADS * HEAD_DIM).astype(jnp.bfloat16)
        grad_values = grad_values.transpose(1, 0, 2).reshape(SEQ_LEN, KV_HEADS * HEAD_DIM).astype(jnp.bfloat16)
        return (grad_queries, grad_keys, grad_values)
    grad_query, grad_key, grad_value = lax.map(one_slab, (query_rows, key_rows, value_rows, teacher_codes, teacher_scales))
    return (grad_query, grad_key, grad_value)
```

```python
import functools
import math

import jax
import jax.numpy as jnp
from jax import lax
from jax.experimental import pallas as pl
from jax.experimental.pallas import tpu as pltpu
from jax.sharding import PartitionSpec as P

HEADS = 16
KV_HEADS = 4
HEAD_DIM = 128
QBLOCK = 128


masked_low = -1e30
QUAD = 4
CHUNKS = 2


def gather_kernel(n_grp, own_ref, all_ref, local_sem, own_sems, z_send, z_recv, x_send, x_recv,
                  y_send, y_recv, d_send, d_recv, r_send, r_recv):
    g = lax.axis_index("grp")
    t = lax.axis_index("tp")
    r = lax.axis_index("rep")
    q = lax.rem(t, QUAD)
    qx = q + 1 - 2 * lax.rem(q, 2)
    qy = lax.rem(q + 2, QUAD)
    qd = lax.rem(qx + 2, QUAD)
    tx = t - q + qx
    ty = t - q + qy
    rows = own_ref.shape[0]
    size = rows // (QUAD * CHUNKS)
    others = n_grp - 1
    to_x, to_y, to_r = {"tp": tx}, {"tp": ty}, {"rep": 1 - r}
    mesh_ids = pl.DeviceIdType.MESH

    barrier = pltpu.get_barrier_semaphore()
    partners = [{"grp": lax.rem(g + k, n_grp)} for k in range(1, n_grp)] + [to_x, to_y, to_r]
    for partner in partners:
        pl.semaphore_signal(barrier, inc=1, device_id=partner, device_id_type=mesh_ids)
    pl.semaphore_wait(barrier, len(partners))

    def spot(quarter, c):
        return pl.ds(pl.multiple_of((quarter * CHUNKS + c) * size, size), size)

    def block(k):
        return lax.rem(g + k, n_grp) * 2 + r

    def sem_at(k, c):
        return c * others + k - 1

    def send(src, dst, sems, index, to):
        return pltpu.make_async_remote_copy(
            src_ref=src, dst_ref=dst, send_sem=sems[0].at[index], recv_sem=sems[1].at[index],
            device_id=to, device_id_type=mesh_ids)

    def forward(k, c, quarter, sems, index, to):
        part = all_ref.at[block(k), spot(quarter, c)]
        return send(part, part, sems, index, to)

    zs, xs, ys, ds, rs = ((z_send, z_recv), (x_send, x_recv), (y_send, y_recv),
                          (d_send, d_recv), (r_send, r_recv))
    started = []

    def go(copy):
        copy.start()
        started.append(copy)

    order = [1, n_grp - 1] + list(range(2, n_grp - 1)) if n_grp > 2 else [1]
    events = [(k, c) for c in range(CHUNKS) for k in order]
    for k, c in events:
        go(send(own_ref.at[spot(q, c)], all_ref.at[block(0), spot(q, c)], zs, sem_at(k, c),
                {"grp": lax.rem(g + n_grp - k, n_grp)}))
    local = pltpu.make_async_copy(own_ref, all_ref.at[block(0)], local_sem.at[0])
    local.start()
    own_swap = pltpu.make_async_remote_copy(
        src_ref=own_ref, dst_ref=all_ref.at[block(0)], send_sem=own_sems.at[0],
        recv_sem=own_sems.at[1], device_id=to_r, device_id_type=mesh_ids)
    own_swap.start()

    swaps = []

    def swap(k, c, quarter, lane):
        copy = forward(k, c, quarter, rs, lane * others * CHUNKS + sem_at(k, c), to_r)
        go(copy)
        swaps.append((k, c, (lane, sem_at(k, c))))

    def on_z(k, c):
        forward(k, c, q, zs, sem_at(k, c), to_x).wait_recv()
        go(forward(k, c, q, xs, sem_at(k, c), to_x))
        go(forward(k, c, q, ys, sem_at(k, c), to_y))
        swap(k, c, q, 0)

    def on_xy(k, c):
        forward(k, c, qx, xs, sem_at(k, c), to_x).wait_recv()
        if events.index((k, c)) % 2 == 0:
            go(forward(k, c, qx, ds, sem_at(k, c), to_y))
        swap(k, c, qx, 1)
        forward(k, c, qy, ys, sem_at(k, c), to_y).wait_recv()
        if events.index((k, c)) % 2 == 1:
            go(forward(k, c, qy, ds, sem_at(k, c), to_x))
        swap(k, c, qy, 2)

    def on_d(k, c):
        forward(k, c, qd, ds, sem_at(k, c), to_x).wait_recv()
        swap(k, c, qd, 3)

    lag = 2
    for i in range(len(events) + 2 * lag):
        if i < len(events):
            on_z(*events[i])
        if lag <= i < len(events) + lag:
            on_xy(*events[i - lag])
        if i >= 2 * lag:
            on_d(*events[i - 2 * lag])

    local.wait()
    own_swap.wait_send()
    for copy in started:
        copy.wait_send()
    peer = all_ref.at[lax.rem(g, n_grp) * 2 + 1 - r]
    pltpu.make_async_remote_copy(
        src_ref=own_ref, dst_ref=peer, send_sem=own_sems.at[0],
        recv_sem=own_sems.at[1], device_id=to_r, device_id_type=mesh_ids).wait_recv()
    for lane, quarter in enumerate((q, qx, qy, qd)):
        for k, c in events:
            part = all_ref.at[lax.rem(g + k, n_grp) * 2 + 1 - r, spot(quarter, c)]
            send(part, part, rs, lane * others * CHUNKS + sem_at(k, c), to_r).wait_recv()


def gather_columns(projection, n_grp, n_rep, n_tp):
    rows, width = projection.shape
    if n_rep != 2 or n_grp < 2 or n_tp % QUAD or rows % (QUAD * CHUNKS * 16):
        return lax.all_gather(projection, ("grp", "rep"), axis=0)
    steps = (n_grp - 1) * CHUNKS
    dma = pltpu.SemaphoreType.DMA
    total = n_grp * n_rep * rows * width
    return pl.pallas_call(
        functools.partial(gather_kernel, n_grp),
        out_shape=jax.ShapeDtypeStruct((n_grp * n_rep, rows, width), projection.dtype),
        in_specs=[pl.BlockSpec(memory_space=pltpu.VMEM)],
        out_specs=pl.BlockSpec(memory_space=pltpu.HBM),
        scratch_shapes=[dma((1,)), dma((2,))] + [dma((steps,))] * 8 + [dma((4 * steps,))] * 2,
        compiler_params=pltpu.CompilerParams(collective_id=0, has_side_effects=True),
        cost_estimate=pl.CostEstimate(flops=0, bytes_accessed=12 * total, transcendentals=0),
    )(projection)


NEAR = 4
SUBS = 4


def fused_kernel(n_grp, n_tp, q_in, k_in, v_in, codes_in, scales_ref, proj_in, dq_ref, dk_ref, dv_ref,
                 q_v, k_all, v_all, codes_v, stage, pq, probs, wide, gathered, acc, errs, terms, sums,
                 pieces, peer_pieces, above, below, lsem, kvz_s, kvz_r, kvd_s, kvd_r, up_s, down_s, z_r,
                 px_s, px_r, pd_s, pd_r, lp_s, ag_s, ag_r, rs_s, rs_r, gd_s, gd_r, gz_s, gz_r):
    g = lax.axis_index("grp")
    t = lax.axis_index("tp")
    r = lax.axis_index("rep")
    rows = q_v.shape[0]
    head_dim = HEAD_DIM
    per = HEADS // KV_HEADS
    feats = per * head_dim
    slabs = codes_v.shape[0]
    width = codes_v.shape[2]
    half = proj_in.shape[1]
    piece = proj_in.shape[0] // n_tp
    sub = piece // SUBS
    length = k_all.shape[0]
    inv_root = 1.0 / math.sqrt(head_dim)
    mesh_ids = pl.DeviceIdType.MESH
    other = {"rep": 1 - r}
    up = {"grp": jnp.minimum(g + 1, n_grp - 1)}
    down = {"grp": jnp.maximum(g - 1, 0)}
    has_up = g < n_grp - 1
    has_down = g > 0

    def peer_tp(m):
        return {"tp": lax.rem(t + m, n_tp)}

    def sender(m):
        return lax.rem(t + n_tp - m, n_tp)

    def send(src, dst, send_sem, recv_sem, to):
        return pltpu.make_async_remote_copy(src_ref=src, dst_ref=dst, send_sem=send_sem, recv_sem=recv_sem,
                                            device_id=to, device_id_type=mesh_ids)

    def arrived(dst, send_sem, recv_sem):
        send(dst, dst, send_sem, recv_sem, other).wait_recv()

    ended = []

    def go(copy, when=None):
        if when is None:
            copy.start()
        else:
            pl.when(when)(copy.start)
        ended.append((copy, when))

    def block(s, core):
        return pl.ds(pl.multiple_of((s * 2 + core) * rows, rows), rows)

    def local(src, dst, index):
        copy = pltpu.make_async_copy(src, dst, lsem.at[index])
        copy.start()
        return copy

    own_k = local(k_in.at[0], k_all.at[block(g, r)], 0)
    own_v = local(v_in.at[0], v_all.at[block(g, r)], 1)
    own_q = local(q_in.at[0], q_v, 2)
    own_codes = local(codes_in, codes_v, 3)
    own_cols = pltpu.make_async_copy(proj_in, pq.at[r], lsem.at[4])
    mine = t == g
    pl.when(mine)(own_cols.start)

    barrier = pltpu.get_barrier_semaphore()
    for to, when in [(other, None), (up, has_up), (down, has_down)] + [(peer_tp(m), None) for m in range(1, n_tp)]:
        def greet(to=to):
            pl.semaphore_signal(barrier, inc=1, device_id=to, device_id_type=mesh_ids)
        if when is None:
            greet()
        else:
            pl.when(when)(greet)
    pl.semaphore_wait(barrier, n_tp + has_up.astype(jnp.int32) + has_down.astype(jnp.int32))

    kv = ((k_in, k_all), (v_in, v_all))
    for i, (src, dst) in enumerate(kv):
        go(send(src.at[0], dst.at[block(g, r)], kvz_s.at[i, g], kvz_r.at[i, g], up), has_up)
    for i, (src, dst) in enumerate(kv):
        go(send(src.at[0], dst.at[block(g, r)], kvd_s.at[i, g], kvd_r.at[i, g], other))

    def own_piece(k):
        return proj_in.at[pl.ds(pl.multiple_of(t * piece + k * sub, sub), sub)]

    def held(s, k):
        return stage.at[s, pl.ds(k * sub, sub)]

    def placed(core, c, k):
        return pq.at[core, pl.ds(pl.multiple_of(c * piece + k * sub, sub), sub)]

    for k in range(SUBS):
        go(send(own_piece(k), held(g, k), down_s.at[g, k], z_r.at[g, k], down), has_down)
    for c in range(n_tp):
        for k in range(SUBS):
            rows_ck = pl.ds(c * piece + k * sub, sub)
            go(send(proj_in.at[rows_ck], placed(r, c, k), pd_s.at[c, k], pd_r.at[c, k], other), mine)

    for s in range(1, n_grp):
        @pl.when(s > g)
        def _():
            span = pl.ds(s * 2 * rows, 2 * rows)
            k_all[span] = jnp.zeros((2 * rows, k_all.shape[1]), k_all.dtype)
            v_all[span] = jnp.zeros((2 * rows, v_all.shape[1]), v_all.dtype)

    own_codes.wait()
    for b in range(width // QBLOCK):
        at = pl.ds(b * QBLOCK, QBLOCK)
        for u in range(slabs):
            acc[u * rows:(u + 1) * rows, at] = -(codes_v[u, :, at].astype(jnp.float32)
                                                * scales_ref[u, :, b:b + 1].astype(jnp.float32))

    for d in range(1, n_grp):
        s = jnp.maximum(g - d, 0)
        here = g >= d
        for i, (_, dst) in enumerate(kv):
            part = dst.at[block(s, r)]
            pl.when(here)(functools.partial(arrived, part, kvz_s.at[i, s], kvz_r.at[i, s]))
            go(send(part, part, kvz_s.at[i, s], kvz_r.at[i, s], up), jnp.logical_and(here, has_up))
            go(send(part, part, kvd_s.at[i, s], kvd_r.at[i, s], other), here)

    def own_up(k):
        go(send(own_piece(k), held(g, k), up_s.at[g, k], z_r.at[g, k], up), has_up)

    for k in range(SUBS // 2):
        own_up(k)

    own_k.wait()
    own_v.wait()
    own_q.wait()
    for s in range(n_grp):
        for i, (_, dst) in enumerate(kv):
            part = dst.at[block(s, 1 - r)]
            pl.when(s <= g)(functools.partial(arrived, part, kvd_s.at[i, s], kvd_r.at[i, s]))

    first = (g * 2 + r) * rows
    row_pos = first + lax.rem(lax.broadcasted_iota(jnp.int32, (per * rows, length), 0), rows)
    allowed = lax.broadcasted_iota(jnp.int32, (per * rows, length), 1) <= row_pos

    def head_cols(kh, j=0):
        return pl.ds(pl.multiple_of(kh * feats + j * head_dim, head_dim), head_dim)

    def kv_cols(kh):
        return pl.ds(pl.multiple_of(kh * head_dim, head_dim), head_dim)

    def stacked_queries(kh):
        return jnp.concatenate([q_v[:, head_cols(kh, j)] for j in range(per)], axis=0)

    def ag_copy(kh, m):
        part = gathered.at[t, kh]
        return send(part, part, ag_s.at[m - 1, kh], ag_r.at[m - 1, kh], peer_tp(m))

    def forward(kh, carry):
        scores = lax.dot_general(stacked_queries(kh), k_all[:, kv_cols(kh)], (((1,), (1,)), ((), ())),
                                 preferred_element_type=jnp.float32) * inv_root
        scores = jnp.where(allowed, scores, masked_low)
        shifted = jnp.exp(scores - scores.max(-1, keepdims=True))
        low = (shifted / shifted.sum(-1, keepdims=True)).astype(jnp.bfloat16)
        probs[kh] = low
        out = jnp.dot(low, v_all[:, kv_cols(kh)], preferred_element_type=jnp.float32)
        wide[kh] = out
        out_low = out.astype(jnp.bfloat16)
        for j in range(per):
            gathered[t, kh, :, j * head_dim:(j + 1) * head_dim] = out_low[j * rows:(j + 1) * rows]
        for m in range(1, n_tp):
            ag_copy(kh, m).start()
        return carry

    lax.fori_loop(0, KV_HEADS, forward, 0)

    def pass_on(c, k):
        part = placed(r, c, k)
        arrived(part, px_s.at[0, k], px_r.at[c, k])
        send(part, part, pd_s.at[c, k], pd_r.at[c, k], other).start()

    def others(k):
        for m in range(1, n_tp):
            pass_on(sender(m), k)

    def event(s, here, k, onward, onward_sem, to):
        part = held(s, k)
        pl.when(here)(functools.partial(arrived, part, up_s.at[s, k], z_r.at[s, k]))
        go(send(part, part, onward_sem.at[s, k], z_r.at[s, k], to), jnp.logical_and(here, onward))
        keep = jnp.logical_and(here, s == t)
        give = jnp.logical_and(here, s != t)
        go(send(part, placed(r, t, k), px_s.at[s, k], px_r.at[t, k], {"tp": s}), give)

        @pl.when(keep)
        def _():
            pltpu.make_async_copy(part, placed(r, t, k), lp_s.at[k]).start()
            send(part, placed(r, t, k), pd_s.at[t, k], pd_r.at[t, k], other).start()
            if k > 0:
                others(k - 1)

    def from_above(d, k):
        event(jnp.minimum(g + d, n_grp - 1), g + d < n_grp, k, has_down, down_s, down)

    def from_below(d, k):
        event(jnp.maximum(g - d, 0), g >= d, k, has_up, up_s, up)

    for k in range(SUBS):
        from_above(1, k)
    for k in range(SUBS // 2, SUBS):
        own_up(k)
    for k in range(SUBS):
        for d in range(1, n_grp):
            from_below(d, k)
    for d in range(2, n_grp):
        for k in range(SUBS):
            from_above(d, k)

    foreign = t != g

    @pl.when(foreign)
    def _():
        others(SUBS - 1)
        for k in range(SUBS):
            pltpu.make_async_copy(held(t, k), placed(r, t, k), lp_s.at[k]).wait()

    pl.when(mine)(own_cols.wait)
    for c in range(n_tp):
        for k in range(SUBS):
            arrived(placed(1 - r, c, k), pd_s.at[c, k], pd_r.at[c, k])

    def proj_rows(kh):
        return pl.ds(pl.multiple_of(kh * feats, feats), feats)

    def project(kh, carry):
        for m in range(1, n_tp):
            arrived(gathered.at[sender(m), kh], ag_s.at[m - 1, kh], ag_r.at[m - 1, kh])
        left = jnp.concatenate([gathered[u, kh] for u in range(slabs)], axis=0)
        for b in range(2):
            acc[:, b * half:(b + 1) * half] += jnp.dot(left, pq[b, proj_rows(kh)],
                                                       preferred_element_type=jnp.float32)
        return carry

    lax.fori_loop(0, KV_HEADS, project, 0)
    errs[...] = acc[...].astype(jnp.bfloat16)

    def rs_copy(kh, m):
        return send(terms.at[kh, lax.rem(t + m, n_tp)], sums.at[kh, m - 1], rs_s.at[m - 1, kh],
                    rs_r.at[m - 1, kh], peer_tp(m))

    def back_project(kh, carry):
        total = jnp.zeros((slabs * rows, feats), jnp.float32)
        for b in range(2):
            total += lax.dot_general(errs[:, b * half:(b + 1) * half], pq[b, proj_rows(kh)],
                                     (((1,), (1,)), ((), ())), preferred_element_type=jnp.float32)
        for u in range(slabs):
            terms[kh, u] = total[u * rows:(u + 1) * rows].astype(jnp.bfloat16)
        for m in range(1, n_tp):
            rs_copy(kh, m).start()
        return carry

    lax.fori_loop(0, KV_HEADS, back_project, 0)

    def gd_copy(kh):
        return send(pieces.at[kh, 1 - r], peer_pieces.at[kh], gd_s.at[kh], gd_r.at[kh], other)

    def backward(kh):
        grad = terms[kh, t].astype(jnp.float32)
        for m in range(1, n_tp):
            arrived(sums.at[kh, m - 1], rs_s.at[m - 1, kh], rs_r.at[m - 1, kh])
            grad += sums[kh, m - 1].astype(jnp.float32)
        grad = grad.astype(jnp.bfloat16)
        grad = jnp.concatenate([grad[:, j * head_dim:(j + 1) * head_dim] for j in range(per)], axis=0)
        delta = (grad.astype(jnp.float32) * wide[kh]).sum(-1, keepdims=True)
        low = probs[kh]
        grad_prob = lax.dot_general(grad, v_all[:, kv_cols(kh)], (((1,), (1,)), ((), ())),
                                    preferred_element_type=jnp.float32)
        score = (low.astype(jnp.float32) * (grad_prob - delta) * inv_root).astype(jnp.bfloat16)
        dq = jnp.dot(score, k_all[:, kv_cols(kh)], preferred_element_type=jnp.float32).astype(jnp.bfloat16)
        for j in range(per):
            dq_ref[0, :, head_cols(kh, j)] = dq[j * rows:(j + 1) * rows]
        over_rows = (((0,), (0,)), ((), ()))
        for i, (lhs, rhs) in enumerate(((stacked_queries(kh), score), (grad, low))):
            term = lax.dot_general(lhs, rhs, over_rows, preferred_element_type=jnp.float32).astype(jnp.bfloat16)
            for s in range(n_grp):
                for core in range(2):
                    at = (s * 2 + core) * rows
                    pieces[kh, core, s, i * head_dim:(i + 1) * head_dim, :] = term[:, at:at + rows]
        gd_copy(kh).start()

    def gz_copy(kh, s):
        return send(below.at[kh, s], above.at[kh, s], gz_s.at[kh, s], gz_r.at[kh, s], down)

    def reduce(kh):
        arrived(peer_pieces.at[kh], gd_s.at[kh], gd_r.at[kh])
        for s in range(n_grp):
            @pl.when(s <= g)
            def _():
                total = pieces[kh, r, s].astype(jnp.float32) + peer_pieces[kh, s].astype(jnp.float32)
                wide_sum[...] = total

                @pl.when(has_up)
                def _():
                    arrived(above.at[kh, s], gz_s.at[kh, s], gz_r.at[kh, s])
                    wide_sum[...] += above[kh, s].astype(jnp.float32)

                @pl.when(s < g)
                def _():
                    below[kh, s] = wide_sum[...].astype(jnp.bfloat16)
                    gz_copy(kh, s).start()

                @pl.when(s == g)
                def _():
                    done = wide_sum[...]
                    dk_ref[0, :, kv_cols(kh)] = done[:head_dim].T.astype(jnp.bfloat16)
                    dv_ref[0, :, kv_cols(kh)] = done[head_dim:].T.astype(jnp.bfloat16)

    def last(kh, carry):
        pl.when(kh < KV_HEADS)(lambda: backward(kh))
        pl.when(kh > 0)(lambda: reduce(kh - 1))
        return carry

    wide_sum = acc.at[pl.ds(0, 2 * head_dim), pl.ds(0, rows)]
    lax.fori_loop(0, KV_HEADS + 1, last, 0)

    for copy, when in ended:
        if when is None:
            copy.wait_send()
        else:
            pl.when(when)(copy.wait_send)

    @pl.when(foreign)
    def _():
        for c in range(n_tp):
            for k in range(SUBS):
                part = placed(r, c, k)
                send(part, part, pd_s.at[c, k], pd_r.at[c, k], other).wait_send()

    def sent(kh, carry):
        for m in range(1, n_tp):
            ag_copy(kh, m).wait_send()
            rs_copy(kh, m).wait_send()
        gd_copy(kh).wait_send()
        for s in range(n_grp):
            pl.when(s < g)(lambda s=s: gz_copy(kh, s).wait_send())
        return carry

    lax.fori_loop(0, KV_HEADS, sent, 0)


def fused(mesh, query_rows, key_rows, value_rows, teacher_codes, teacher_scales, projection):
    n_grp, n_tp = mesh.shape["grp"], mesh.shape["tp"]
    rows, depth = query_rows.shape[1:]
    kv_width = key_rows.shape[2]
    slabs, _, width = teacher_codes.shape
    half = projection.shape[1]
    length = n_grp * 2 * rows
    per = HEADS // KV_HEADS
    feats = per * HEAD_DIM
    piece = depth // n_tp
    low, wide = jnp.bfloat16, jnp.float32
    vmem = pltpu.VMEM
    dma = pltpu.SemaphoreType.DMA
    hbm_spec = pl.BlockSpec(memory_space=pl.ANY)
    vmem_spec = pl.BlockSpec(memory_space=pltpu.VMEM)
    scratch = [
        vmem((rows, depth), low), vmem((length, kv_width), low), vmem((length, kv_width), low),
        vmem((slabs, rows, width), low), vmem((n_grp, piece, half), low), vmem((2, depth, half), low),
        vmem((KV_HEADS, per * rows, length), low), vmem((KV_HEADS, per * rows, HEAD_DIM), wide),
        vmem((slabs, KV_HEADS, rows, feats), low), vmem((slabs * rows, width), wide),
        vmem((slabs * rows, width), low), vmem((KV_HEADS, slabs, rows, feats), low),
        vmem((KV_HEADS, n_tp - 1, rows, feats), low), vmem((KV_HEADS, 2, n_grp, 2 * HEAD_DIM, rows), low),
        vmem((KV_HEADS, n_grp, 2 * HEAD_DIM, rows), low), vmem((KV_HEADS, n_grp, 2 * HEAD_DIM, rows), low),
        vmem((KV_HEADS, n_grp, 2 * HEAD_DIM, rows), low),
        dma((5,)), dma((2, n_grp)), dma((2, n_grp)), dma((2, n_grp)), dma((2, n_grp)),
        dma((n_grp, SUBS)), dma((n_grp, SUBS)), dma((n_grp, SUBS)),
        dma((n_grp, SUBS)), dma((n_tp, SUBS)), dma((n_tp, SUBS)), dma((n_tp, SUBS)), dma((SUBS,)),
        dma((n_tp - 1, KV_HEADS)), dma((n_tp - 1, KV_HEADS)), dma((n_tp - 1, KV_HEADS)),
        dma((n_tp - 1, KV_HEADS)), dma((KV_HEADS,)), dma((KV_HEADS,)),
        dma((KV_HEADS, n_grp)), dma((KV_HEADS, n_grp)),
    ]
    return pl.pallas_call(
        functools.partial(fused_kernel, n_grp, n_tp),
        out_shape=[jax.ShapeDtypeStruct(a.shape, a.dtype) for a in (query_rows, key_rows, value_rows)],
        in_specs=[hbm_spec] * 4 + [vmem_spec, hbm_spec],
        out_specs=[vmem_spec] * 3,
        scratch_shapes=scratch,
        compiler_params=pltpu.CompilerParams(collective_id=1, has_side_effects=True,
                                             vmem_limit_bytes=60 * 2 ** 20),
    )(query_rows, key_rows, value_rows, teacher_codes, teacher_scales, projection)


def suits(mesh, teacher_codes, projection):
    depth, half = projection.shape
    n_grp, n_tp, n_rep = (mesh.shape[axis] for axis in ("grp", "tp", "rep"))
    return (n_rep == 2 and 1 < n_grp == n_tp <= NEAR and teacher_codes.shape[2] == 2 * half
            and depth % (n_tp * SUBS * 16) == 0)


def shards(mesh, query_rows, key_rows, value_rows, teacher_codes, teacher_scales, projection):
    if suits(mesh, teacher_codes, projection):
        return tuple(fused(mesh, query_rows, key_rows, value_rows, teacher_codes, teacher_scales, projection))
    rows_dev = query_rows.shape[1]
    group_size = HEADS // KV_HEADS
    inv_root = 1.0 / math.sqrt(HEAD_DIM)
    kv_width = key_rows.shape[2]
    pairs_all = lax.all_gather(
        jnp.concatenate([key_rows, value_rows], 2), ("grp", "rep"), axis=1, tiled=True
    )
    keys_all, values_all = pairs_all[..., :kv_width], pairs_all[..., kv_width:]
    length = keys_all.shape[1]
    my_index = lax.axis_index(("grp", "rep"))
    first_row = my_index * rows_dev
    queries = query_rows[0].reshape(rows_dev, KV_HEADS, group_size, HEAD_DIM).transpose(1, 2, 0, 3)
    key_heads = keys_all[0].reshape(length, KV_HEADS, HEAD_DIM).transpose(1, 0, 2)
    value_heads = values_all[0].reshape(length, KV_HEADS, HEAD_DIM).transpose(1, 0, 2)
    row_pos = first_row + jnp.arange(rows_dev, dtype=jnp.int32)
    slab_codes, slab_scales = (
        lax.all_to_all(teacher_codes, "tp", split_axis=0, concat_axis=2, tiled=True),
        lax.all_to_all(teacher_scales, "tp", split_axis=0, concat_axis=2, tiled=True),
    )

    raw_scores = (
        jnp.einsum("hgqd,hkd->hgqk", queries, key_heads, preferred_element_type=jnp.float32)
        * inv_root
    )
    allowed = jnp.arange(length, dtype=jnp.int32)[None, :] <= row_pos[:, None]
    scores = jnp.where(allowed, raw_scores, masked_low)
    row_peak = scores.max(-1, keepdims=True)
    shifted = jnp.exp(scores - row_peak)
    probs = shifted / shifted.sum(-1, keepdims=True)
    prob_low = probs.astype(jnp.bfloat16)
    attn_wide = jnp.einsum(
        "hgqk,hkd->hgqd", prob_low, value_heads, preferred_element_type=jnp.float32
    )
    attn_low = (
        attn_wide.transpose(2, 0, 1, 3).reshape(rows_dev, HEADS * HEAD_DIM).astype(jnp.bfloat16)
    )
    col_width = projection.shape[1]
    shaped = gather_columns(
        projection, mesh.shape["grp"], mesh.shape["rep"], mesh.shape["tp"]
    )
    pieces = shaped.shape[0]
    approx = jnp.einsum("td,sdc->tsc", attn_low, shaped, preferred_element_type=jnp.float32)
    code_rows = slab_codes[0].astype(jnp.float32)
    scale_rows = slab_scales[0].astype(jnp.float32)
    target = (code_rows.reshape(rows_dev, -1, QBLOCK) * scale_rows[..., None]).reshape(
        rows_dev, pieces, col_width
    )
    errors = (approx - target).astype(jnp.bfloat16)
    partial_terms = jnp.einsum(
        "tsc,sdc->std", errors, shaped, preferred_element_type=jnp.float32
    ).astype(jnp.bfloat16)
    grad_attn = partial_terms.astype(jnp.float32).sum(0)
    grad_low = grad_attn.astype(jnp.bfloat16)
    grad_heads = grad_low.reshape(rows_dev, KV_HEADS, group_size, HEAD_DIM).transpose(1, 2, 0, 3)
    row_delta = (grad_heads.astype(jnp.float32) * attn_wide).sum(-1)

    grad_values = jnp.einsum(
        "hgqk,hgqd->hkd", prob_low, grad_heads, preferred_element_type=jnp.float32
    )
    grad_prob = jnp.einsum(
        "hgqd,hkd->hgqk", grad_heads, value_heads, preferred_element_type=jnp.float32
    )
    grad_score = (probs * (grad_prob - row_delta[..., None]) * inv_root).astype(jnp.bfloat16)
    grad_queries = jnp.einsum(
        "hgqk,hkd->hgqd", grad_score, key_heads, preferred_element_type=jnp.float32
    )
    grad_keys = jnp.einsum(
        "hgqk,hgqd->hkd", grad_score, queries, preferred_element_type=jnp.float32
    )
    key_terms = grad_keys.transpose(1, 0, 2).reshape(1, length, KV_HEADS * HEAD_DIM)
    value_terms = grad_values.transpose(1, 0, 2).reshape(1, length, KV_HEADS * HEAD_DIM)
    pair_terms = jnp.concatenate([key_terms, value_terms], 2).astype(jnp.bfloat16)
    pair_grad = lax.psum_scatter(
        pair_terms, ("grp", "rep"), scatter_dimension=1, tiled=True
    )
    key_grad, value_grad = pair_grad[..., :kv_width], pair_grad[..., kv_width:]
    query_grad = (
        grad_queries.transpose(2, 0, 1, 3)
        .reshape(1, rows_dev, HEADS * HEAD_DIM)
        .astype(jnp.bfloat16)
    )
    return (query_grad, key_grad.astype(jnp.bfloat16), value_grad.astype(jnp.bfloat16))


def solution(mesh):
    placed = (
        P("tp", ("grp", "rep"), None),
        P("tp", ("grp", "rep"), None),
        P("tp", ("grp", "rep"), None),
        P(None, ("grp", "rep"), "tp"),
        P(None, ("grp", "rep"), "tp"),
        P(None, ("grp", "rep")),
    )
    return jax.shard_map(
        functools.partial(shards, mesh),
        mesh=mesh,
        in_specs=placed,
        out_specs=(
            P("tp", ("grp", "rep"), None),
            P("tp", ("grp", "rep"), None),
            P("tp", ("grp", "rep"), None),
        ),
        check_vma=False,
    )
```

```python
import functools
import math

import jax
import jax.numpy as jnp
from jax import lax
from jax.experimental import pallas as pl
from jax.experimental.pallas import tpu as pltpu
from jax.sharding import PartitionSpec as P

HEADS = 16
KV_HEADS = 4
HEAD_DIM = 128
QBLOCK = 128


masked_low = -1e30
QUAD = 4
CHUNKS = 2


def gather_kernel(n_grp, own_ref, all_ref, local_sem, own_sems, z_send, z_recv, x_send, x_recv,
                  y_send, y_recv, d_send, d_recv, r_send, r_recv):
    g = lax.axis_index("grp")
    t = lax.axis_index("tp")
    r = lax.axis_index("rep")
    q = lax.rem(t, QUAD)
    qx = q + 1 - 2 * lax.rem(q, 2)
    qy = lax.rem(q + 2, QUAD)
    qd = lax.rem(qx + 2, QUAD)
    tx = t - q + qx
    ty = t - q + qy
    rows = own_ref.shape[0]
    size = rows // (QUAD * CHUNKS)
    others = n_grp - 1
    to_x, to_y, to_r = {"tp": tx}, {"tp": ty}, {"rep": 1 - r}
    mesh_ids = pl.DeviceIdType.MESH

    barrier = pltpu.get_barrier_semaphore()
    partners = [{"grp": lax.rem(g + k, n_grp)} for k in range(1, n_grp)] + [to_x, to_y, to_r]
    for partner in partners:
        pl.semaphore_signal(barrier, inc=1, device_id=partner, device_id_type=mesh_ids)
    pl.semaphore_wait(barrier, len(partners))

    def spot(quarter, c):
        return pl.ds(pl.multiple_of((quarter * CHUNKS + c) * size, size), size)

    def block(k):
        return lax.rem(g + k, n_grp) * 2 + r

    def sem_at(k, c):
        return c * others + k - 1

    def send(src, dst, sems, index, to):
        return pltpu.make_async_remote_copy(
            src_ref=src, dst_ref=dst, send_sem=sems[0].at[index], recv_sem=sems[1].at[index],
            device_id=to, device_id_type=mesh_ids)

    def forward(k, c, quarter, sems, index, to):
        part = all_ref.at[block(k), spot(quarter, c)]
        return send(part, part, sems, index, to)

    zs, xs, ys, ds, rs = ((z_send, z_recv), (x_send, x_recv), (y_send, y_recv),
                          (d_send, d_recv), (r_send, r_recv))
    started = []

    def go(copy):
        copy.start()
        started.append(copy)

    order = [1, n_grp - 1] + list(range(2, n_grp - 1)) if n_grp > 2 else [1]
    events = [(k, c) for c in range(CHUNKS) for k in order]
    for k, c in events:
        go(send(own_ref.at[spot(q, c)], all_ref.at[block(0), spot(q, c)], zs, sem_at(k, c),
                {"grp": lax.rem(g + n_grp - k, n_grp)}))
    local = pltpu.make_async_copy(own_ref, all_ref.at[block(0)], local_sem.at[0])
    local.start()
    own_swap = pltpu.make_async_remote_copy(
        src_ref=own_ref, dst_ref=all_ref.at[block(0)], send_sem=own_sems.at[0],
        recv_sem=own_sems.at[1], device_id=to_r, device_id_type=mesh_ids)
    own_swap.start()

    swaps = []

    def swap(k, c, quarter, lane):
        copy = forward(k, c, quarter, rs, lane * others * CHUNKS + sem_at(k, c), to_r)
        go(copy)
        swaps.append((k, c, (lane, sem_at(k, c))))

    def on_z(k, c):
        forward(k, c, q, zs, sem_at(k, c), to_x).wait_recv()
        go(forward(k, c, q, xs, sem_at(k, c), to_x))
        go(forward(k, c, q, ys, sem_at(k, c), to_y))
        swap(k, c, q, 0)

    def on_xy(k, c):
        forward(k, c, qx, xs, sem_at(k, c), to_x).wait_recv()
        if events.index((k, c)) % 2 == 0:
            go(forward(k, c, qx, ds, sem_at(k, c), to_y))
        swap(k, c, qx, 1)
        forward(k, c, qy, ys, sem_at(k, c), to_y).wait_recv()
        if events.index((k, c)) % 2 == 1:
            go(forward(k, c, qy, ds, sem_at(k, c), to_x))
        swap(k, c, qy, 2)

    def on_d(k, c):
        forward(k, c, qd, ds, sem_at(k, c), to_x).wait_recv()
        swap(k, c, qd, 3)

    lag = 2
    for i in range(len(events) + 2 * lag):
        if i < len(events):
            on_z(*events[i])
        if lag <= i < len(events) + lag:
            on_xy(*events[i - lag])
        if i >= 2 * lag:
            on_d(*events[i - 2 * lag])

    local.wait()
    own_swap.wait_send()
    for copy in started:
        copy.wait_send()
    peer = all_ref.at[lax.rem(g, n_grp) * 2 + 1 - r]
    pltpu.make_async_remote_copy(
        src_ref=own_ref, dst_ref=peer, send_sem=own_sems.at[0],
        recv_sem=own_sems.at[1], device_id=to_r, device_id_type=mesh_ids).wait_recv()
    for lane, quarter in enumerate((q, qx, qy, qd)):
        for k, c in events:
            part = all_ref.at[lax.rem(g + k, n_grp) * 2 + 1 - r, spot(quarter, c)]
            send(part, part, rs, lane * others * CHUNKS + sem_at(k, c), to_r).wait_recv()


def gather_columns(projection, n_grp, n_rep, n_tp):
    rows, width = projection.shape
    if n_rep != 2 or n_grp < 2 or n_tp % QUAD or rows % (QUAD * CHUNKS * 16):
        return lax.all_gather(projection, ("grp", "rep"), axis=0)
    steps = (n_grp - 1) * CHUNKS
    dma = pltpu.SemaphoreType.DMA
    total = n_grp * n_rep * rows * width
    return pl.pallas_call(
        functools.partial(gather_kernel, n_grp),
        out_shape=jax.ShapeDtypeStruct((n_grp * n_rep, rows, width), projection.dtype),
        in_specs=[pl.BlockSpec(memory_space=pltpu.VMEM)],
        out_specs=pl.BlockSpec(memory_space=pltpu.HBM),
        scratch_shapes=[dma((1,)), dma((2,))] + [dma((steps,))] * 8 + [dma((4 * steps,))] * 2,
        compiler_params=pltpu.CompilerParams(collective_id=0, has_side_effects=True),
        cost_estimate=pl.CostEstimate(flops=0, bytes_accessed=12 * total, transcendentals=0),
    )(projection)


NEAR = 4
SUBS = 4


def fused_kernel(n_grp, n_tp, q_in, k_in, v_in, codes_in, scales_in, proj_in, dq_ref, dk_ref, dv_ref,
                 q_v, k_all, v_all, codes_v, scales_ref, pq, probs, wide, gathered, acc, errs, terms, sums,
                 pieces, peer_pieces, above, below, lsem, kvz_s, kvz_r, kvd_s, kvd_r, up_s, down_s, z_r,
                 pd_s, pd_r, ag_s, ag_r, rs_s, rs_r, gd_s, gd_r, gz_s, gz_r):
    g = lax.axis_index("grp")
    t = lax.axis_index("tp")
    r = lax.axis_index("rep")
    rows = q_v.shape[0]
    head_dim = HEAD_DIM
    per = HEADS // KV_HEADS
    feats = per * head_dim
    slabs = codes_v.shape[0]
    width = codes_v.shape[2]
    half = proj_in.shape[1]
    steps = KV_HEADS * SUBS
    sub = proj_in.shape[0] // steps
    length = k_all.shape[0]
    inv_root = 1.0 / math.sqrt(head_dim)
    mesh_ids = pl.DeviceIdType.MESH
    other = {"rep": 1 - r}
    up = {"grp": jnp.minimum(g + 1, n_grp - 1)}
    down = {"grp": jnp.maximum(g - 1, 0)}
    has_up = g < n_grp - 1
    has_down = g > 0

    def peer_tp(m):
        return {"tp": lax.rem(t + m, n_tp)}

    def sender(m):
        return lax.rem(t + n_tp - m, n_tp)

    def send(src, dst, send_sem, recv_sem, to):
        return pltpu.make_async_remote_copy(src_ref=src, dst_ref=dst, send_sem=send_sem, recv_sem=recv_sem,
                                            device_id=to, device_id_type=mesh_ids)

    def arrived(dst, send_sem, recv_sem):
        send(dst, dst, send_sem, recv_sem, other).wait_recv()

    ended = []

    def go(copy, when=None):
        if when is None:
            copy.start()
        else:
            pl.when(when)(copy.start)
        ended.append((copy, when))

    def block(s, core):
        return pl.ds(pl.multiple_of((s * 2 + core) * rows, rows), rows)

    def local(src, dst, index):
        copy = pltpu.make_async_copy(src, dst, lsem.at[index])
        copy.start()
        return copy

    own_k = local(k_in.at[0], k_all.at[block(g, r)], 0)
    own_v = local(v_in.at[0], v_all.at[block(g, r)], 1)
    own_q = local(q_in.at[0], q_v, 2)
    own_codes = local(codes_in, codes_v, 3)
    own_scales = local(scales_in, scales_ref, 4)
    own_cols = pltpu.make_async_copy(proj_in, pq.at[r], lsem.at[5])
    mine = t == g
    pl.when(mine)(own_cols.start)

    barrier = pltpu.get_barrier_semaphore()
    greeted = [other] + [peer_tp(m) for m in range(1, n_tp)] + [{"grp": lax.rem(g + m, n_grp)} for m in range(1, n_grp)]
    for to in greeted:
        pl.semaphore_signal(barrier, inc=1, device_id=to, device_id_type=mesh_ids)
    pl.semaphore_wait(barrier, len(greeted))

    kv = ((k_in, k_all), (v_in, v_all))
    for i, (src, dst) in enumerate(kv):
        go(send(src.at[0], dst.at[block(g, r)], kvz_s.at[i, g], kvz_r.at[i, g], up), has_up)
    for i, (src, dst) in enumerate(kv):
        go(send(src.at[0], dst.at[block(g, r)], kvd_s.at[i, g], kvd_r.at[i, g], other))

    def span(k):
        return pl.ds(k * sub if isinstance(k, int) else pl.multiple_of(k * sub, sub), sub)

    def placed(core, k):
        return pq.at[core, span(k)]

    def own_down(k):
        return send(proj_in.at[span(k)], placed(r, k), down_s.at[k], z_r.at[k], down)

    def own_up(k):
        return send(proj_in.at[span(k)], placed(r, k), up_s.at[k], z_r.at[k], up)

    def own_over(k):
        return send(proj_in.at[span(k)], placed(r, k), pd_s.at[k], pd_r.at[k], other)

    for k in range(steps):
        go(own_down(k), jnp.logical_and(mine, has_down))
    for k in range(steps):
        go(own_over(k), mine)

    for s in range(1, n_grp):
        @pl.when(s > g)
        def _():
            unseen = pl.ds(s * 2 * rows, 2 * rows)
            k_all[unseen] = jnp.zeros((2 * rows, k_all.shape[1]), k_all.dtype)
            v_all[unseen] = jnp.zeros((2 * rows, v_all.shape[1]), v_all.dtype)

    own_codes.wait()
    own_scales.wait()
    scales = [scales_ref[u].astype(jnp.float32).T for u in range(slabs)]
    for b in range(width // QBLOCK):
        at = pl.ds(b * QBLOCK, QBLOCK)
        for u in range(slabs):
            acc[u * rows:(u + 1) * rows, at] = -(codes_v[u, :, at].astype(jnp.float32) * scales[u][:, b:b + 1])

    for d in range(1, n_grp):
        s = jnp.maximum(g - d, 0)
        here = g >= d
        for i, (_, dst) in enumerate(kv):
            part = dst.at[block(s, r)]
            pl.when(here)(functools.partial(arrived, part, kvz_s.at[i, s], kvz_r.at[i, s]))
            go(send(part, part, kvz_s.at[i, s], kvz_r.at[i, s], up), jnp.logical_and(here, has_up))
            go(send(part, part, kvd_s.at[i, s], kvd_r.at[i, s], other), here)

    for k in range(steps):
        go(own_up(k), jnp.logical_and(mine, has_up))

    own_k.wait()
    own_v.wait()
    own_q.wait()
    for s in range(n_grp):
        for i, (_, dst) in enumerate(kv):
            part = dst.at[block(s, 1 - r)]
            pl.when(s <= g)(functools.partial(arrived, part, kvd_s.at[i, s], kvd_r.at[i, s]))

    first = (g * 2 + r) * rows
    row_pos = first + lax.rem(lax.broadcasted_iota(jnp.int32, (per * rows, length), 0), rows)
    allowed = lax.broadcasted_iota(jnp.int32, (per * rows, length), 1) <= row_pos

    def head_cols(kh, j=0):
        return pl.ds(pl.multiple_of(kh * feats + j * head_dim, head_dim), head_dim)

    def kv_cols(kh):
        return pl.ds(pl.multiple_of(kh * head_dim, head_dim), head_dim)

    def stacked_queries(kh):
        return jnp.concatenate([q_v[:, head_cols(kh, j)] for j in range(per)], axis=0)

    def ag_copy(kh, m):
        part = gathered.at[t, kh]
        return send(part, part, ag_s.at[m - 1, kh], ag_r.at[m - 1, kh], peer_tp(m))

    def forward(kh, carry):
        scores = lax.dot_general(stacked_queries(kh), k_all[:, kv_cols(kh)], (((1,), (1,)), ((), ())),
                                 preferred_element_type=jnp.float32) * inv_root
        scores = jnp.where(allowed, scores, masked_low)
        shifted = jnp.exp(scores - scores.max(-1, keepdims=True))
        low = (shifted / shifted.sum(-1, keepdims=True)).astype(jnp.bfloat16)
        probs[kh] = low
        out = jnp.dot(low, v_all[:, kv_cols(kh)], preferred_element_type=jnp.float32)
        wide[kh] = out
        out_low = out.astype(jnp.bfloat16)
        for j in range(per):
            gathered[t, kh, :, j * head_dim:(j + 1) * head_dim] = out_low[j * rows:(j + 1) * rows]
        for m in range(1, n_tp):
            ag_copy(kh, m).start()
        return carry

    lax.fori_loop(0, KV_HEADS, forward, 0)

    rising = t < g
    falling = t > g
    onward_up = jnp.logical_and(rising, has_up)
    onward_down = jnp.logical_and(falling, has_down)
    onward = jnp.logical_or(onward_up, onward_down)
    foreign = t != g

    def relay_up(k):
        return send(placed(r, k), placed(r, k), up_s.at[k], z_r.at[k], up)

    def relay_down(k):
        return send(placed(r, k), placed(r, k), down_s.at[k], z_r.at[k], down)

    def relay_over(k):
        return send(placed(r, k), placed(r, k), pd_s.at[k], pd_r.at[k], other)

    def proj_rows(kh):
        return pl.ds(pl.multiple_of(kh * feats, feats), feats)

    def receive(kh):
        for i in range(SUBS):
            k = kh * SUBS + i
            arrived(placed(r, k), up_s.at[k], z_r.at[k])
            pl.when(onward_up)(lambda k=k: relay_up(k).start())
            pl.when(onward_down)(lambda k=k: relay_down(k).start())
            relay_over(k).start()

    def project(kh):
        for m in range(1, n_tp):
            arrived(gathered.at[sender(m), kh], ag_s.at[m - 1, kh], ag_r.at[m - 1, kh])
        for i in range(SUBS):
            k = kh * SUBS + i
            arrived(placed(1 - r, k), pd_s.at[k], pd_r.at[k])
        left = jnp.concatenate([gathered[u, kh] for u in range(slabs)], axis=0)
        for b in range(2):
            acc[:, b * half:(b + 1) * half] += jnp.dot(left, pq[b, proj_rows(kh)],
                                                       preferred_element_type=jnp.float32)

    pl.when(mine)(own_cols.wait)
    behind = jnp.where(onward, KV_HEADS, 0)

    def collect(i, carry):
        pl.when(jnp.logical_and(foreign, i < KV_HEADS))(lambda: receive(i))
        pl.when(i >= behind)(lambda: project(i - behind))
        return carry

    lax.fori_loop(0, KV_HEADS + behind, collect, 0)
    errs[...] = acc[...].astype(jnp.bfloat16)

    def rs_copy(kh, m):
        return send(terms.at[kh, lax.rem(t + m, n_tp)], sums.at[kh, m - 1], rs_s.at[m - 1, kh],
                    rs_r.at[m - 1, kh], peer_tp(m))

    def back_project(kh, carry):
        total = jnp.zeros((slabs * rows, feats), jnp.float32)
        for b in range(2):
            total += lax.dot_general(errs[:, b * half:(b + 1) * half], pq[b, proj_rows(kh)],
                                     (((1,), (1,)), ((), ())), preferred_element_type=jnp.float32)
        for u in range(slabs):
            terms[kh, u] = total[u * rows:(u + 1) * rows].astype(jnp.bfloat16)
        for m in range(1, n_tp):
            rs_copy(kh, m).start()
        return carry

    lax.fori_loop(0, KV_HEADS, back_project, 0)

    def gd_copy(kh):
        return send(pieces.at[kh, 1 - r], peer_pieces.at[kh], gd_s.at[kh], gd_r.at[kh], other)

    def backward(kh):
        grad = terms[kh, t].astype(jnp.float32)
        for m in range(1, n_tp):
            arrived(sums.at[kh, m - 1], rs_s.at[m - 1, kh], rs_r.at[m - 1, kh])
            grad += sums[kh, m - 1].astype(jnp.float32)
        grad = grad.astype(jnp.bfloat16)
        grad = jnp.concatenate([grad[:, j * head_dim:(j + 1) * head_dim] for j in range(per)], axis=0)
        delta = (grad.astype(jnp.float32) * wide[kh]).sum(-1, keepdims=True)
        low = probs[kh]
        grad_prob = lax.dot_general(grad, v_all[:, kv_cols(kh)], (((1,), (1,)), ((), ())),
                                    preferred_element_type=jnp.float32)
        score = (low.astype(jnp.float32) * (grad_prob - delta) * inv_root).astype(jnp.bfloat16)
        dq = jnp.dot(score, k_all[:, kv_cols(kh)], preferred_element_type=jnp.float32).astype(jnp.bfloat16)
        for j in range(per):
            dq_ref[0, :, head_cols(kh, j)] = dq[j * rows:(j + 1) * rows]
        over_rows = (((0,), (0,)), ((), ()))
        for i, (lhs, rhs) in enumerate(((stacked_queries(kh), score), (grad, low))):
            term = lax.dot_general(lhs, rhs, over_rows, preferred_element_type=jnp.float32).astype(jnp.bfloat16)
            for s in range(n_grp):
                for core in range(2):
                    at = (s * 2 + core) * rows
                    pieces[kh, core, s, i * head_dim:(i + 1) * head_dim, :] = term[:, at:at + rows]
        gd_copy(kh).start()

    def gz_copy(kh, s):
        return send(below.at[kh, s], above.at[kh, g], gz_s.at[kh, s], gz_r.at[kh, g], {"grp": s})

    def both_cores(kh, s):
        return pieces[kh, r, s].astype(jnp.float32) + peer_pieces[kh, s].astype(jnp.float32)

    def hand_down(kh):
        arrived(peer_pieces.at[kh], gd_s.at[kh], gd_r.at[kh])
        for s in range(n_grp - 1):
            @pl.when(s < g)
            def _():
                below[kh, s] = both_cores(kh, s).astype(jnp.bfloat16)
                gz_copy(kh, s).start()

    def settle(kh):
        wide_sum[...] = both_cores(kh, g)
        for s in range(1, n_grp):
            @pl.when(s > g)
            def _():
                arrived(above.at[kh, s], gz_s.at[kh, s], gz_r.at[kh, s])
                wide_sum[...] += above[kh, s].astype(jnp.float32)
        done = wide_sum[...]
        dk_ref[0, :, kv_cols(kh)] = done[:head_dim].T.astype(jnp.bfloat16)
        dv_ref[0, :, kv_cols(kh)] = done[head_dim:].T.astype(jnp.bfloat16)

    def last(kh, carry):
        backward(kh)
        hand_down(kh)
        return carry

    def finish(kh, carry):
        settle(kh)
        return carry

    wide_sum = acc.at[pl.ds(0, 2 * head_dim), pl.ds(0, rows)]
    lax.fori_loop(0, KV_HEADS, last, 0)
    lax.fori_loop(0, KV_HEADS, finish, 0)

    for copy, when in ended:
        if when is None:
            copy.wait_send()
        else:
            pl.when(when)(copy.wait_send)

    def relayed(k, carry):
        relay_over(k).wait_send()
        pl.when(onward_up)(lambda: relay_up(k).wait_send())
        pl.when(onward_down)(lambda: relay_down(k).wait_send())
        return carry

    pl.when(foreign)(lambda: lax.fori_loop(0, steps, relayed, None))

    def sent(kh, carry):
        for m in range(1, n_tp):
            ag_copy(kh, m).wait_send()
            rs_copy(kh, m).wait_send()
        gd_copy(kh).wait_send()
        for s in range(n_grp - 1):
            pl.when(s < g)(lambda s=s: gz_copy(kh, s).wait_send())
        return carry

    lax.fori_loop(0, KV_HEADS, sent, 0)


def hand_out(dq_in, dk_in, dv_in, dq_out, dk_out, dv_out, sems):
    pairs = ((dq_in, dq_out), (dk_in, dk_out), (dv_in, dv_out))
    copies = [pltpu.make_async_copy(src, dst, sems.at[i]) for i, (src, dst) in enumerate(pairs)]
    for copy in copies:
        copy.start()
    for copy in copies:
        copy.wait()


def fused(mesh, query_rows, key_rows, value_rows, teacher_codes, teacher_scales, projection):
    n_grp, n_tp = mesh.shape["grp"], mesh.shape["tp"]
    rows, depth = query_rows.shape[1:]
    kv_width = key_rows.shape[2]
    slabs, _, width = teacher_codes.shape
    half = projection.shape[1]
    length = n_grp * 2 * rows
    per = HEADS // KV_HEADS
    feats = per * HEAD_DIM
    steps = KV_HEADS * SUBS
    low, wide = jnp.bfloat16, jnp.float32
    vmem = pltpu.VMEM
    dma = pltpu.SemaphoreType.DMA
    hbm_spec = pl.BlockSpec(memory_space=pltpu.HBM)
    flat_scales = teacher_scales.transpose(0, 2, 1)
    vmem_spec = pl.BlockSpec(memory_space=pltpu.VMEM)
    scratch = [
        vmem((rows, depth), low), vmem((length, kv_width), low), vmem((length, kv_width), low),
        vmem((slabs, rows, width), low), vmem(flat_scales.shape, low), vmem((2, depth, half), low),
        vmem((KV_HEADS, per * rows, length), low), vmem((KV_HEADS, per * rows, HEAD_DIM), wide),
        vmem((slabs, KV_HEADS, rows, feats), low), vmem((slabs * rows, width), wide),
        vmem((slabs * rows, width), low), vmem((KV_HEADS, slabs, rows, feats), low),
        vmem((KV_HEADS, n_tp - 1, rows, feats), low), vmem((KV_HEADS, 2, n_grp, 2 * HEAD_DIM, rows), low),
        vmem((KV_HEADS, n_grp, 2 * HEAD_DIM, rows), low), vmem((KV_HEADS, n_grp, 2 * HEAD_DIM, rows), low),
        vmem((KV_HEADS, n_grp, 2 * HEAD_DIM, rows), low),
        dma((6,)), dma((2, n_grp)), dma((2, n_grp)), dma((2, n_grp)), dma((2, n_grp)),
        dma((steps,)), dma((steps,)), dma((steps,)), dma((steps,)), dma((steps,)),
        dma((n_tp - 1, KV_HEADS)), dma((n_tp - 1, KV_HEADS)), dma((n_tp - 1, KV_HEADS)),
        dma((n_tp - 1, KV_HEADS)), dma((KV_HEADS,)), dma((KV_HEADS,)),
        dma((KV_HEADS, n_grp)), dma((KV_HEADS, n_grp)),
    ]
    outs = [jax.ShapeDtypeStruct(a.shape, a.dtype) for a in (query_rows, key_rows, value_rows)]
    grads = pl.pallas_call(
        functools.partial(fused_kernel, n_grp, n_tp),
        out_shape=outs,
        in_specs=[hbm_spec] * 6,
        out_specs=[vmem_spec] * 3,
        scratch_shapes=scratch,
        compiler_params=pltpu.CompilerParams(collective_id=1, has_side_effects=True,
                                             vmem_limit_bytes=60 * 2 ** 20),
    )(query_rows, key_rows, value_rows, teacher_codes, flat_scales, projection)
    return pl.pallas_call(
        hand_out,
        out_shape=outs,
        in_specs=[pl.BlockSpec(memory_space=pl.ANY)] * 3,
        out_specs=[hbm_spec] * 3,
        scratch_shapes=[dma((len(outs),))],
        compiler_params=pltpu.CompilerParams(vmem_limit_bytes=2 ** 20),
    )(*grads)


def suits(mesh, teacher_codes, projection):
    depth, half = projection.shape
    n_grp, n_tp, n_rep = (mesh.shape[axis] for axis in ("grp", "tp", "rep"))
    return (n_rep == 2 and 1 < n_grp == n_tp <= NEAR and teacher_codes.shape[2] == 2 * half
            and depth % (KV_HEADS * SUBS * 16) == 0)


def shards(mesh, query_rows, key_rows, value_rows, teacher_codes, teacher_scales, projection):
    if suits(mesh, teacher_codes, projection):
        return tuple(fused(mesh, query_rows, key_rows, value_rows, teacher_codes, teacher_scales, projection))
    rows_dev = query_rows.shape[1]
    group_size = HEADS // KV_HEADS
    inv_root = 1.0 / math.sqrt(HEAD_DIM)
    kv_width = key_rows.shape[2]
    pairs_all = lax.all_gather(
        jnp.concatenate([key_rows, value_rows], 2), ("grp", "rep"), axis=1, tiled=True
    )
    keys_all, values_all = pairs_all[..., :kv_width], pairs_all[..., kv_width:]
    length = keys_all.shape[1]
    my_index = lax.axis_index(("grp", "rep"))
    first_row = my_index * rows_dev
    queries = query_rows[0].reshape(rows_dev, KV_HEADS, group_size, HEAD_DIM).transpose(1, 2, 0, 3)
    key_heads = keys_all[0].reshape(length, KV_HEADS, HEAD_DIM).transpose(1, 0, 2)
    value_heads = values_all[0].reshape(length, KV_HEADS, HEAD_DIM).transpose(1, 0, 2)
    row_pos = first_row + jnp.arange(rows_dev, dtype=jnp.int32)
    slab_codes, slab_scales = (
        lax.all_to_all(teacher_codes, "tp", split_axis=0, concat_axis=2, tiled=True),
        lax.all_to_all(teacher_scales, "tp", split_axis=0, concat_axis=2, tiled=True),
    )

    raw_scores = (
        jnp.einsum("hgqd,hkd->hgqk", queries, key_heads, preferred_element_type=jnp.float32)
        * inv_root
    )
    allowed = jnp.arange(length, dtype=jnp.int32)[None, :] <= row_pos[:, None]
    scores = jnp.where(allowed, raw_scores, masked_low)
    row_peak = scores.max(-1, keepdims=True)
    shifted = jnp.exp(scores - row_peak)
    probs = shifted / shifted.sum(-1, keepdims=True)
    prob_low = probs.astype(jnp.bfloat16)
    attn_wide = jnp.einsum(
        "hgqk,hkd->hgqd", prob_low, value_heads, preferred_element_type=jnp.float32
    )
    attn_low = (
        attn_wide.transpose(2, 0, 1, 3).reshape(rows_dev, HEADS * HEAD_DIM).astype(jnp.bfloat16)
    )
    col_width = projection.shape[1]
    shaped = gather_columns(
        projection, mesh.shape["grp"], mesh.shape["rep"], mesh.shape["tp"]
    )
    pieces = shaped.shape[0]
    approx = jnp.einsum("td,sdc->tsc", attn_low, shaped, preferred_element_type=jnp.float32)
    code_rows = slab_codes[0].astype(jnp.float32)
    scale_rows = slab_scales[0].astype(jnp.float32)
    target = (code_rows.reshape(rows_dev, -1, QBLOCK) * scale_rows[..., None]).reshape(
        rows_dev, pieces, col_width
    )
    errors = (approx - target).astype(jnp.bfloat16)
    partial_terms = jnp.einsum(
        "tsc,sdc->std", errors, shaped, preferred_element_type=jnp.float32
    ).astype(jnp.bfloat16)
    grad_attn = partial_terms.astype(jnp.float32).sum(0)
    grad_low = grad_attn.astype(jnp.bfloat16)
    grad_heads = grad_low.reshape(rows_dev, KV_HEADS, group_size, HEAD_DIM).transpose(1, 2, 0, 3)
    row_delta = (grad_heads.astype(jnp.float32) * attn_wide).sum(-1)

    grad_values = jnp.einsum(
        "hgqk,hgqd->hkd", prob_low, grad_heads, preferred_element_type=jnp.float32
    )
    grad_prob = jnp.einsum(
        "hgqd,hkd->hgqk", grad_heads, value_heads, preferred_element_type=jnp.float32
    )
    grad_score = (probs * (grad_prob - row_delta[..., None]) * inv_root).astype(jnp.bfloat16)
    grad_queries = jnp.einsum(
        "hgqk,hkd->hgqd", grad_score, key_heads, preferred_element_type=jnp.float32
    )
    grad_keys = jnp.einsum(
        "hgqk,hgqd->hkd", grad_score, queries, preferred_element_type=jnp.float32
    )
    key_terms = grad_keys.transpose(1, 0, 2).reshape(1, length, KV_HEADS * HEAD_DIM)
    value_terms = grad_values.transpose(1, 0, 2).reshape(1, length, KV_HEADS * HEAD_DIM)
    pair_terms = jnp.concatenate([key_terms, value_terms], 2).astype(jnp.bfloat16)
    pair_grad = lax.psum_scatter(
        pair_terms, ("grp", "rep"), scatter_dimension=1, tiled=True
    )
    key_grad, value_grad = pair_grad[..., :kv_width], pair_grad[..., kv_width:]
    query_grad = (
        grad_queries.transpose(2, 0, 1, 3)
        .reshape(1, rows_dev, HEADS * HEAD_DIM)
        .astype(jnp.bfloat16)
    )
    return (query_grad, key_grad.astype(jnp.bfloat16), value_grad.astype(jnp.bfloat16))


def solution(mesh):
    placed = (
        P("tp", ("grp", "rep"), None),
        P("tp", ("grp", "rep"), None),
        P("tp", ("grp", "rep"), None),
        P(None, ("grp", "rep"), "tp"),
        P(None, ("grp", "rep"), "tp"),
        P(None, ("grp", "rep")),
    )
    return jax.shard_map(
        functools.partial(shards, mesh),
        mesh=mesh,
        in_specs=placed,
        out_specs=(
            P("tp", ("grp", "rep"), None),
            P("tp", ("grp", "rep"), None),
            P("tp", ("grp", "rep"), None),
        ),
        check_vma=False,
    )
```

```python
import functools
import math

import jax
import jax.numpy as jnp
from jax import lax
from jax.experimental import pallas as pl
from jax.experimental.pallas import tpu as pltpu
from jax.sharding import PartitionSpec as P

HEADS = 16
KV_HEADS = 4
HEAD_DIM = 128
QBLOCK = 128


masked_low = -1e30
QUAD = 4
CHUNKS = 2


def gather_kernel(n_grp, own_ref, all_ref, local_sem, own_sems, z_send, z_recv, x_send, x_recv,
                  y_send, y_recv, d_send, d_recv, r_send, r_recv):
    g = lax.axis_index("grp")
    t = lax.axis_index("tp")
    r = lax.axis_index("rep")
    q = lax.rem(t, QUAD)
    qx = q + 1 - 2 * lax.rem(q, 2)
    qy = lax.rem(q + 2, QUAD)
    qd = lax.rem(qx + 2, QUAD)
    tx = t - q + qx
    ty = t - q + qy
    rows = own_ref.shape[0]
    size = rows // (QUAD * CHUNKS)
    others = n_grp - 1
    to_x, to_y, to_r = {"tp": tx}, {"tp": ty}, {"rep": 1 - r}
    mesh_ids = pl.DeviceIdType.MESH

    barrier = pltpu.get_barrier_semaphore()
    partners = [{"grp": lax.rem(g + k, n_grp)} for k in range(1, n_grp)] + [to_x, to_y, to_r]
    for partner in partners:
        pl.semaphore_signal(barrier, inc=1, device_id=partner, device_id_type=mesh_ids)
    pl.semaphore_wait(barrier, len(partners))

    def spot(quarter, c):
        return pl.ds(pl.multiple_of((quarter * CHUNKS + c) * size, size), size)

    def block(k):
        return lax.rem(g + k, n_grp) * 2 + r

    def sem_at(k, c):
        return c * others + k - 1

    def send(src, dst, sems, index, to):
        return pltpu.make_async_remote_copy(
            src_ref=src, dst_ref=dst, send_sem=sems[0].at[index], recv_sem=sems[1].at[index],
            device_id=to, device_id_type=mesh_ids)

    def forward(k, c, quarter, sems, index, to):
        part = all_ref.at[block(k), spot(quarter, c)]
        return send(part, part, sems, index, to)

    zs, xs, ys, ds, rs = ((z_send, z_recv), (x_send, x_recv), (y_send, y_recv),
                          (d_send, d_recv), (r_send, r_recv))
    started = []

    def go(copy):
        copy.start()
        started.append(copy)

    order = [1, n_grp - 1] + list(range(2, n_grp - 1)) if n_grp > 2 else [1]
    events = [(k, c) for c in range(CHUNKS) for k in order]
    for k, c in events:
        go(send(own_ref.at[spot(q, c)], all_ref.at[block(0), spot(q, c)], zs, sem_at(k, c),
                {"grp": lax.rem(g + n_grp - k, n_grp)}))
    local = pltpu.make_async_copy(own_ref, all_ref.at[block(0)], local_sem.at[0])
    local.start()
    own_swap = pltpu.make_async_remote_copy(
        src_ref=own_ref, dst_ref=all_ref.at[block(0)], send_sem=own_sems.at[0],
        recv_sem=own_sems.at[1], device_id=to_r, device_id_type=mesh_ids)
    own_swap.start()

    swaps = []

    def swap(k, c, quarter, lane):
        copy = forward(k, c, quarter, rs, lane * others * CHUNKS + sem_at(k, c), to_r)
        go(copy)
        swaps.append((k, c, (lane, sem_at(k, c))))

    def on_z(k, c):
        forward(k, c, q, zs, sem_at(k, c), to_x).wait_recv()
        go(forward(k, c, q, xs, sem_at(k, c), to_x))
        go(forward(k, c, q, ys, sem_at(k, c), to_y))
        swap(k, c, q, 0)

    def on_xy(k, c):
        forward(k, c, qx, xs, sem_at(k, c), to_x).wait_recv()
        if events.index((k, c)) % 2 == 0:
            go(forward(k, c, qx, ds, sem_at(k, c), to_y))
        swap(k, c, qx, 1)
        forward(k, c, qy, ys, sem_at(k, c), to_y).wait_recv()
        if events.index((k, c)) % 2 == 1:
            go(forward(k, c, qy, ds, sem_at(k, c), to_x))
        swap(k, c, qy, 2)

    def on_d(k, c):
        forward(k, c, qd, ds, sem_at(k, c), to_x).wait_recv()
        swap(k, c, qd, 3)

    lag = 2
    for i in range(len(events) + 2 * lag):
        if i < len(events):
            on_z(*events[i])
        if lag <= i < len(events) + lag:
            on_xy(*events[i - lag])
        if i >= 2 * lag:
            on_d(*events[i - 2 * lag])

    local.wait()
    own_swap.wait_send()
    for copy in started:
        copy.wait_send()
    peer = all_ref.at[lax.rem(g, n_grp) * 2 + 1 - r]
    pltpu.make_async_remote_copy(
        src_ref=own_ref, dst_ref=peer, send_sem=own_sems.at[0],
        recv_sem=own_sems.at[1], device_id=to_r, device_id_type=mesh_ids).wait_recv()
    for lane, quarter in enumerate((q, qx, qy, qd)):
        for k, c in events:
            part = all_ref.at[lax.rem(g + k, n_grp) * 2 + 1 - r, spot(quarter, c)]
            send(part, part, rs, lane * others * CHUNKS + sem_at(k, c), to_r).wait_recv()


def gather_columns(projection, n_grp, n_rep, n_tp):
    rows, width = projection.shape
    if n_rep != 2 or n_grp < 2 or n_tp % QUAD or rows % (QUAD * CHUNKS * 16):
        return lax.all_gather(projection, ("grp", "rep"), axis=0)
    steps = (n_grp - 1) * CHUNKS
    dma = pltpu.SemaphoreType.DMA
    total = n_grp * n_rep * rows * width
    return pl.pallas_call(
        functools.partial(gather_kernel, n_grp),
        out_shape=jax.ShapeDtypeStruct((n_grp * n_rep, rows, width), projection.dtype),
        in_specs=[pl.BlockSpec(memory_space=pltpu.VMEM)],
        out_specs=pl.BlockSpec(memory_space=pltpu.HBM),
        scratch_shapes=[dma((1,)), dma((2,))] + [dma((steps,))] * 8 + [dma((4 * steps,))] * 2,
        compiler_params=pltpu.CompilerParams(collective_id=0, has_side_effects=True),
        cost_estimate=pl.CostEstimate(flops=0, bytes_accessed=12 * total, transcendentals=0),
    )(projection)


NEAR = 4
SUBS = 4


def fused_kernel(n_grp, n_tp, q_in, k_in, v_in, codes_in, scales_in, proj_in, dq_ref, dk_ref, dv_ref,
                 q_v, k_all, v_all, codes_v, scales_ref, pq, probs, wide, gathered, acc, errs, terms, sums,
                 pieces, peer_pieces, above, below, lsem, kvz_s, kvz_r, kvd_s, kvd_r, up_s, down_s, z_r,
                 pd_s, pd_r, ag_s, ag_r, rs_s, rs_r, gd_s, gd_r, gz_s, gz_r):
    g = lax.axis_index("grp")
    t = lax.axis_index("tp")
    r = lax.axis_index("rep")
    rows = q_v.shape[0]
    head_dim = HEAD_DIM
    per = HEADS // KV_HEADS
    feats = per * head_dim
    slabs = codes_v.shape[0]
    width = codes_v.shape[2]
    half = proj_in.shape[1]
    steps = KV_HEADS * SUBS
    sub = proj_in.shape[0] // steps
    length = k_all.shape[0]
    inv_root = 1.0 / math.sqrt(head_dim)
    mesh_ids = pl.DeviceIdType.MESH
    other = {"rep": 1 - r}
    up = {"grp": jnp.minimum(g + 1, n_grp - 1)}
    down = {"grp": jnp.maximum(g - 1, 0)}
    has_up = g < n_grp - 1
    has_down = g > 0

    def peer_tp(m):
        return {"tp": lax.rem(t + m, n_tp)}

    def sender(m):
        return lax.rem(t + n_tp - m, n_tp)

    def send(src, dst, send_sem, recv_sem, to):
        return pltpu.make_async_remote_copy(src_ref=src, dst_ref=dst, send_sem=send_sem, recv_sem=recv_sem,
                                            device_id=to, device_id_type=mesh_ids)

    def arrived(dst, send_sem, recv_sem):
        send(dst, dst, send_sem, recv_sem, other).wait_recv()

    ended = []

    def go(copy, when=None):
        if when is None:
            copy.start()
        else:
            pl.when(when)(copy.start)
        ended.append((copy, when))

    def block(s, core):
        return pl.ds(pl.multiple_of((s * 2 + core) * rows, rows), rows)

    def local(src, dst, index):
        copy = pltpu.make_async_copy(src, dst, lsem.at[index])
        copy.start()
        return copy

    own_k = local(k_in.at[0], k_all.at[block(g, r)], 0)
    own_v = local(v_in.at[0], v_all.at[block(g, r)], 1)
    own_q = local(q_in.at[0], q_v, 2)
    own_codes = local(codes_in, codes_v, 3)
    own_scales = local(scales_in, scales_ref, 4)
    own_cols = pltpu.make_async_copy(proj_in, pq.at[r], lsem.at[5])
    mine = t == g
    pl.when(mine)(own_cols.start)

    barrier = pltpu.get_barrier_semaphore()
    greeted = [other] + [peer_tp(m) for m in range(1, n_tp)] + [{"grp": lax.rem(g + m, n_grp)} for m in range(1, n_grp)]
    for to in greeted:
        pl.semaphore_signal(barrier, inc=1, device_id=to, device_id_type=mesh_ids)
    pl.semaphore_wait(barrier, len(greeted))

    kv = ((k_in, k_all), (v_in, v_all))
    for i, (src, dst) in enumerate(kv):
        go(send(src.at[0], dst.at[block(g, r)], kvz_s.at[i, g], kvz_r.at[i, g], up), has_up)
    for i, (src, dst) in enumerate(kv):
        go(send(src.at[0], dst.at[block(g, r)], kvd_s.at[i, g], kvd_r.at[i, g], other))

    def span(k):
        return pl.ds(k * sub if isinstance(k, int) else pl.multiple_of(k * sub, sub), sub)

    def placed(core, k):
        return pq.at[core, span(k)]

    def own_down(k):
        return send(proj_in.at[span(k)], placed(r, k), down_s.at[k], z_r.at[k], down)

    def own_up(k):
        return send(proj_in.at[span(k)], placed(r, k), up_s.at[k], z_r.at[k], up)

    def own_over(k):
        return send(proj_in.at[span(k)], placed(r, k), pd_s.at[k], pd_r.at[k], other)

    for k in range(steps):
        go(own_down(k), jnp.logical_and(mine, has_down))
    for k in range(steps):
        go(own_over(k), mine)

    for s in range(1, n_grp):
        @pl.when(s > g)
        def _():
            unseen = pl.ds(s * 2 * rows, 2 * rows)
            k_all[unseen] = jnp.zeros((2 * rows, k_all.shape[1]), k_all.dtype)
            v_all[unseen] = jnp.zeros((2 * rows, v_all.shape[1]), v_all.dtype)

    own_codes.wait()
    own_scales.wait()
    scales = [scales_ref[u].astype(jnp.float32).T for u in range(slabs)]
    for b in range(width // QBLOCK):
        at = pl.ds(b * QBLOCK, QBLOCK)
        for u in range(slabs):
            acc[u * rows:(u + 1) * rows, at] = -(codes_v[u, :, at].astype(jnp.float32) * scales[u][:, b:b + 1])

    for d in range(1, n_grp):
        s = jnp.maximum(g - d, 0)
        here = g >= d
        for i, (_, dst) in enumerate(kv):
            part = dst.at[block(s, r)]
            pl.when(here)(functools.partial(arrived, part, kvz_s.at[i, s], kvz_r.at[i, s]))
            go(send(part, part, kvz_s.at[i, s], kvz_r.at[i, s], up), jnp.logical_and(here, has_up))
            go(send(part, part, kvd_s.at[i, s], kvd_r.at[i, s], other), here)

    for k in range(steps):
        go(own_up(k), jnp.logical_and(mine, has_up))

    own_k.wait()
    own_v.wait()
    own_q.wait()
    for s in range(n_grp):
        for i, (_, dst) in enumerate(kv):
            part = dst.at[block(s, 1 - r)]
            pl.when(s <= g)(functools.partial(arrived, part, kvd_s.at[i, s], kvd_r.at[i, s]))

    first = (g * 2 + r) * rows
    row_pos = first + lax.rem(lax.broadcasted_iota(jnp.int32, (per * rows, length), 0), rows)
    allowed = lax.broadcasted_iota(jnp.int32, (per * rows, length), 1) <= row_pos

    def head_cols(kh, j=0):
        return pl.ds(pl.multiple_of(kh * feats + j * head_dim, head_dim), head_dim)

    def kv_cols(kh):
        return pl.ds(pl.multiple_of(kh * head_dim, head_dim), head_dim)

    def stacked_queries(kh):
        return jnp.concatenate([q_v[:, head_cols(kh, j)] for j in range(per)], axis=0)

    def ag_copy(kh, m):
        part = gathered.at[t, kh]
        return send(part, part, ag_s.at[m - 1, kh], ag_r.at[m - 1, kh], peer_tp(m))

    rising = t < g
    falling = t > g
    onward_up = jnp.logical_and(rising, has_up)
    onward_down = jnp.logical_and(falling, has_down)
    onward = jnp.logical_or(onward_up, onward_down)
    foreign = t != g

    def relay_up(k):
        return send(placed(r, k), placed(r, k), up_s.at[k], z_r.at[k], up)

    def relay_down(k):
        return send(placed(r, k), placed(r, k), down_s.at[k], z_r.at[k], down)

    def relay_over(k):
        return send(placed(r, k), placed(r, k), pd_s.at[k], pd_r.at[k], other)

    def receive_one(k):
        arrived(placed(r, k), up_s.at[k], z_r.at[k])
        pl.when(onward_up)(lambda: relay_up(k).start())
        pl.when(onward_down)(lambda: relay_down(k).start())
        relay_over(k).start()

    def receive(kh):
        for i in range(SUBS):
            receive_one(kh * SUBS + i)

    def forward(kh, carry):
        pl.when(onward)(lambda: receive_one(kh))
        scores = lax.dot_general(stacked_queries(kh), k_all[:, kv_cols(kh)], (((1,), (1,)), ((), ())),
                                 preferred_element_type=jnp.float32) * inv_root
        scores = jnp.where(allowed, scores, masked_low)
        shifted = jnp.exp(scores - scores.max(-1, keepdims=True))
        low = (shifted / shifted.sum(-1, keepdims=True)).astype(jnp.bfloat16)
        probs[kh] = low
        out = jnp.dot(low, v_all[:, kv_cols(kh)], preferred_element_type=jnp.float32)
        wide[kh] = out
        out_low = out.astype(jnp.bfloat16)
        for j in range(per):
            gathered[t, kh, :, j * head_dim:(j + 1) * head_dim] = out_low[j * rows:(j + 1) * rows]
        for m in range(1, n_tp):
            ag_copy(kh, m).start()
        return carry

    lax.fori_loop(0, KV_HEADS, forward, 0)

    def proj_rows(kh):
        return pl.ds(pl.multiple_of(kh * feats, feats), feats)

    def project(kh):
        for m in range(1, n_tp):
            arrived(gathered.at[sender(m), kh], ag_s.at[m - 1, kh], ag_r.at[m - 1, kh])
        for i in range(SUBS):
            k = kh * SUBS + i
            arrived(placed(1 - r, k), pd_s.at[k], pd_r.at[k])
        left = jnp.concatenate([gathered[u, kh] for u in range(slabs)], axis=0)
        for b in range(2):
            acc[:, b * half:(b + 1) * half] += jnp.dot(left, pq[b, proj_rows(kh)],
                                                       preferred_element_type=jnp.float32)

    pl.when(mine)(own_cols.wait)
    behind = jnp.where(onward, KV_HEADS, 0)

    def collect(i, carry):
        pl.when(jnp.logical_and(jnp.logical_and(foreign, i < KV_HEADS), jnp.logical_or(i > 0, jnp.logical_not(onward))))(lambda: receive(i))
        pl.when(i >= behind)(lambda: project(i - behind))
        return carry

    lax.fori_loop(0, KV_HEADS + behind, collect, 0)
    errs[...] = acc[...].astype(jnp.bfloat16)

    def rs_copy(kh, m):
        return send(terms.at[kh, lax.rem(t + m, n_tp)], sums.at[kh, m - 1], rs_s.at[m - 1, kh],
                    rs_r.at[m - 1, kh], peer_tp(m))

    def back_project(kh, carry):
        total = jnp.zeros((slabs * rows, feats), jnp.float32)
        for b in range(2):
            total += lax.dot_general(errs[:, b * half:(b + 1) * half], pq[b, proj_rows(kh)],
                                     (((1,), (1,)), ((), ())), preferred_element_type=jnp.float32)
        for u in range(slabs):
            terms[kh, u] = total[u * rows:(u + 1) * rows].astype(jnp.bfloat16)
        for m in range(1, n_tp):
            rs_copy(kh, m).start()
        return carry

    lax.fori_loop(0, KV_HEADS, back_project, 0)

    def gd_copy(kh):
        return send(pieces.at[kh, 1 - r], peer_pieces.at[kh], gd_s.at[kh], gd_r.at[kh], other)

    def backward(kh):
        grad = terms[kh, t].astype(jnp.float32)
        for m in range(1, n_tp):
            arrived(sums.at[kh, m - 1], rs_s.at[m - 1, kh], rs_r.at[m - 1, kh])
            grad += sums[kh, m - 1].astype(jnp.float32)
        grad = grad.astype(jnp.bfloat16)
        grad = jnp.concatenate([grad[:, j * head_dim:(j + 1) * head_dim] for j in range(per)], axis=0)
        delta = (grad.astype(jnp.float32) * wide[kh]).sum(-1, keepdims=True)
        low = probs[kh]
        grad_prob = lax.dot_general(grad, v_all[:, kv_cols(kh)], (((1,), (1,)), ((), ())),
                                    preferred_element_type=jnp.float32)
        score = (low.astype(jnp.float32) * (grad_prob - delta) * inv_root).astype(jnp.bfloat16)
        dq = jnp.dot(score, k_all[:, kv_cols(kh)], preferred_element_type=jnp.float32).astype(jnp.bfloat16)
        for j in range(per):
            dq_ref[0, :, head_cols(kh, j)] = dq[j * rows:(j + 1) * rows]
        over_rows = (((0,), (0,)), ((), ()))
        for i, (lhs, rhs) in enumerate(((stacked_queries(kh), score), (grad, low))):
            term = lax.dot_general(lhs, rhs, over_rows, preferred_element_type=jnp.float32).astype(jnp.bfloat16)
            for s in range(n_grp):
                for core in range(2):
                    at = (s * 2 + core) * rows
                    pieces[kh, core, s, i * head_dim:(i + 1) * head_dim, :] = term[:, at:at + rows]
        gd_copy(kh).start()

    def gz_copy(kh, s):
        return send(below.at[kh, s], above.at[kh, g], gz_s.at[kh, s], gz_r.at[kh, g], {"grp": s})

    def both_cores(kh, s):
        return pieces[kh, r, s].astype(jnp.float32) + peer_pieces[kh, s].astype(jnp.float32)

    def hand_down(kh):
        arrived(peer_pieces.at[kh], gd_s.at[kh], gd_r.at[kh])
        for s in range(n_grp - 1):
            @pl.when(s < g)
            def _():
                below[kh, s] = both_cores(kh, s).astype(jnp.bfloat16)
                gz_copy(kh, s).start()

    def settle(kh):
        wide_sum[...] = both_cores(kh, g)
        for s in range(1, n_grp):
            @pl.when(s > g)
            def _():
                arrived(above.at[kh, s], gz_s.at[kh, s], gz_r.at[kh, s])
                wide_sum[...] += above[kh, s].astype(jnp.float32)
        done = wide_sum[...]
        dk_ref[0, :, kv_cols(kh)] = done[:head_dim].T.astype(jnp.bfloat16)
        dv_ref[0, :, kv_cols(kh)] = done[head_dim:].T.astype(jnp.bfloat16)

    def last(kh, carry):
        backward(kh)
        hand_down(kh)
        return carry

    def finish(kh, carry):
        settle(kh)
        return carry

    wide_sum = acc.at[pl.ds(0, 2 * head_dim), pl.ds(0, rows)]
    lax.fori_loop(0, KV_HEADS, last, 0)
    lax.fori_loop(0, KV_HEADS, finish, 0)

    for copy, when in ended:
        if when is None:
            copy.wait_send()
        else:
            pl.when(when)(copy.wait_send)

    def relayed(k, carry):
        relay_over(k).wait_send()
        pl.when(onward_up)(lambda: relay_up(k).wait_send())
        pl.when(onward_down)(lambda: relay_down(k).wait_send())
        return carry

    pl.when(foreign)(lambda: lax.fori_loop(0, steps, relayed, None))

    def sent(kh, carry):
        for m in range(1, n_tp):
            ag_copy(kh, m).wait_send()
            rs_copy(kh, m).wait_send()
        gd_copy(kh).wait_send()
        for s in range(n_grp - 1):
            pl.when(s < g)(lambda s=s: gz_copy(kh, s).wait_send())
        return carry

    lax.fori_loop(0, KV_HEADS, sent, 0)


def hand_out(dq_in, dk_in, dv_in, dq_out, dk_out, dv_out, sems):
    pairs = ((dq_in, dq_out), (dk_in, dk_out), (dv_in, dv_out))
    copies = [pltpu.make_async_copy(src, dst, sems.at[i]) for i, (src, dst) in enumerate(pairs)]
    for copy in copies:
        copy.start()
    for copy in copies:
        copy.wait()


def fused(mesh, query_rows, key_rows, value_rows, teacher_codes, teacher_scales, projection):
    n_grp, n_tp = mesh.shape["grp"], mesh.shape["tp"]
    rows, depth = query_rows.shape[1:]
    kv_width = key_rows.shape[2]
    slabs, _, width = teacher_codes.shape
    half = projection.shape[1]
    length = n_grp * 2 * rows
    per = HEADS // KV_HEADS
    feats = per * HEAD_DIM
    steps = KV_HEADS * SUBS
    low, wide = jnp.bfloat16, jnp.float32
    vmem = pltpu.VMEM
    dma = pltpu.SemaphoreType.DMA
    hbm_spec = pl.BlockSpec(memory_space=pltpu.HBM)
    flat_scales = teacher_scales.transpose(0, 2, 1)
    vmem_spec = pl.BlockSpec(memory_space=pltpu.VMEM)
    scratch = [
        vmem((rows, depth), low), vmem((length, kv_width), low), vmem((length, kv_width), low),
        vmem((slabs, rows, width), low), vmem(flat_scales.shape, low), vmem((2, depth, half), low),
        vmem((KV_HEADS, per * rows, length), low), vmem((KV_HEADS, per * rows, HEAD_DIM), wide),
        vmem((slabs, KV_HEADS, rows, feats), low), vmem((slabs * rows, width), wide),
        vmem((slabs * rows, width), low), vmem((KV_HEADS, slabs, rows, feats), low),
        vmem((KV_HEADS, n_tp - 1, rows, feats), low), vmem((KV_HEADS, 2, n_grp, 2 * HEAD_DIM, rows), low),
        vmem((KV_HEADS, n_grp, 2 * HEAD_DIM, rows), low), vmem((KV_HEADS, n_grp, 2 * HEAD_DIM, rows), low),
        vmem((KV_HEADS, n_grp, 2 * HEAD_DIM, rows), low),
        dma((6,)), dma((2, n_grp)), dma((2, n_grp)), dma((2, n_grp)), dma((2, n_grp)),
        dma((steps,)), dma((steps,)), dma((steps,)), dma((steps,)), dma((steps,)),
        dma((n_tp - 1, KV_HEADS)), dma((n_tp - 1, KV_HEADS)), dma((n_tp - 1, KV_HEADS)),
        dma((n_tp - 1, KV_HEADS)), dma((KV_HEADS,)), dma((KV_HEADS,)),
        dma((KV_HEADS, n_grp)), dma((KV_HEADS, n_grp)),
    ]
    outs = [jax.ShapeDtypeStruct(a.shape, a.dtype) for a in (query_rows, key_rows, value_rows)]
    grads = pl.pallas_call(
        functools.partial(fused_kernel, n_grp, n_tp),
        out_shape=outs,
        in_specs=[hbm_spec] * 6,
        out_specs=[vmem_spec] * 3,
        scratch_shapes=scratch,
        compiler_params=pltpu.CompilerParams(collective_id=1, has_side_effects=True,
                                             vmem_limit_bytes=60 * 2 ** 20),
    )(query_rows, key_rows, value_rows, teacher_codes, flat_scales, projection)
    return pl.pallas_call(
        hand_out,
        out_shape=outs,
        in_specs=[pl.BlockSpec(memory_space=pl.ANY)] * 3,
        out_specs=[hbm_spec] * 3,
        scratch_shapes=[dma((len(outs),))],
        compiler_params=pltpu.CompilerParams(vmem_limit_bytes=2 ** 20),
    )(*grads)


def suits(mesh, teacher_codes, projection):
    depth, half = projection.shape
    n_grp, n_tp, n_rep = (mesh.shape[axis] for axis in ("grp", "tp", "rep"))
    return (n_rep == 2 and 1 < n_grp == n_tp <= NEAR and teacher_codes.shape[2] == 2 * half
            and depth % (KV_HEADS * SUBS * 16) == 0)


def shards(mesh, query_rows, key_rows, value_rows, teacher_codes, teacher_scales, projection):
    if suits(mesh, teacher_codes, projection):
        return tuple(fused(mesh, query_rows, key_rows, value_rows, teacher_codes, teacher_scales, projection))
    rows_dev = query_rows.shape[1]
    group_size = HEADS // KV_HEADS
    inv_root = 1.0 / math.sqrt(HEAD_DIM)
    kv_width = key_rows.shape[2]
    pairs_all = lax.all_gather(
        jnp.concatenate([key_rows, value_rows], 2), ("grp", "rep"), axis=1, tiled=True
    )
    keys_all, values_all = pairs_all[..., :kv_width], pairs_all[..., kv_width:]
    length = keys_all.shape[1]
    my_index = lax.axis_index(("grp", "rep"))
    first_row = my_index * rows_dev
    queries = query_rows[0].reshape(rows_dev, KV_HEADS, group_size, HEAD_DIM).transpose(1, 2, 0, 3)
    key_heads = keys_all[0].reshape(length, KV_HEADS, HEAD_DIM).transpose(1, 0, 2)
    value_heads = values_all[0].reshape(length, KV_HEADS, HEAD_DIM).transpose(1, 0, 2)
    row_pos = first_row + jnp.arange(rows_dev, dtype=jnp.int32)
    slab_codes, slab_scales = (
        lax.all_to_all(teacher_codes, "tp", split_axis=0, concat_axis=2, tiled=True),
        lax.all_to_all(teacher_scales, "tp", split_axis=0, concat_axis=2, tiled=True),
    )

    raw_scores = (
        jnp.einsum("hgqd,hkd->hgqk", queries, key_heads, preferred_element_type=jnp.float32)
        * inv_root
    )
    allowed = jnp.arange(length, dtype=jnp.int32)[None, :] <= row_pos[:, None]
    scores = jnp.where(allowed, raw_scores, masked_low)
    row_peak = scores.max(-1, keepdims=True)
    shifted = jnp.exp(scores - row_peak)
    probs = shifted / shifted.sum(-1, keepdims=True)
    prob_low = probs.astype(jnp.bfloat16)
    attn_wide = jnp.einsum(
        "hgqk,hkd->hgqd", prob_low, value_heads, preferred_element_type=jnp.float32
    )
    attn_low = (
        attn_wide.transpose(2, 0, 1, 3).reshape(rows_dev, HEADS * HEAD_DIM).astype(jnp.bfloat16)
    )
    col_width = projection.shape[1]
    shaped = gather_columns(
        projection, mesh.shape["grp"], mesh.shape["rep"], mesh.shape["tp"]
    )
    pieces = shaped.shape[0]
    approx = jnp.einsum("td,sdc->tsc", attn_low, shaped, preferred_element_type=jnp.float32)
    code_rows = slab_codes[0].astype(jnp.float32)
    scale_rows = slab_scales[0].astype(jnp.float32)
    target = (code_rows.reshape(rows_dev, -1, QBLOCK) * scale_rows[..., None]).reshape(
        rows_dev, pieces, col_width
    )
    errors = (approx - target).astype(jnp.bfloat16)
    partial_terms = jnp.einsum(
        "tsc,sdc->std", errors, shaped, preferred_element_type=jnp.float32
    ).astype(jnp.bfloat16)
    grad_attn = partial_terms.astype(jnp.float32).sum(0)
    grad_low = grad_attn.astype(jnp.bfloat16)
    grad_heads = grad_low.reshape(rows_dev, KV_HEADS, group_size, HEAD_DIM).transpose(1, 2, 0, 3)
    row_delta = (grad_heads.astype(jnp.float32) * attn_wide).sum(-1)

    grad_values = jnp.einsum(
        "hgqk,hgqd->hkd", prob_low, grad_heads, preferred_element_type=jnp.float32
    )
    grad_prob = jnp.einsum(
        "hgqd,hkd->hgqk", grad_heads, value_heads, preferred_element_type=jnp.float32
    )
    grad_score = (probs * (grad_prob - row_delta[..., None]) * inv_root).astype(jnp.bfloat16)
    grad_queries = jnp.einsum(
        "hgqk,hkd->hgqd", grad_score, key_heads, preferred_element_type=jnp.float32
    )
    grad_keys = jnp.einsum(
        "hgqk,hgqd->hkd", grad_score, queries, preferred_element_type=jnp.float32
    )
    key_terms = grad_keys.transpose(1, 0, 2).reshape(1, length, KV_HEADS * HEAD_DIM)
    value_terms = grad_values.transpose(1, 0, 2).reshape(1, length, KV_HEADS * HEAD_DIM)
    pair_terms = jnp.concatenate([key_terms, value_terms], 2).astype(jnp.bfloat16)
    pair_grad = lax.psum_scatter(
        pair_terms, ("grp", "rep"), scatter_dimension=1, tiled=True
    )
    key_grad, value_grad = pair_grad[..., :kv_width], pair_grad[..., kv_width:]
    query_grad = (
        grad_queries.transpose(2, 0, 1, 3)
        .reshape(1, rows_dev, HEADS * HEAD_DIM)
        .astype(jnp.bfloat16)
    )
    return (query_grad, key_grad.astype(jnp.bfloat16), value_grad.astype(jnp.bfloat16))


def solution(mesh):
    placed = (
        P("tp", ("grp", "rep"), None),
        P("tp", ("grp", "rep"), None),
        P("tp", ("grp", "rep"), None),
        P(None, ("grp", "rep"), "tp"),
        P(None, ("grp", "rep"), "tp"),
        P(None, ("grp", "rep")),
    )
    return jax.shard_map(
        functools.partial(shards, mesh),
        mesh=mesh,
        in_specs=placed,
        out_specs=(
            P("tp", ("grp", "rep"), None),
            P("tp", ("grp", "rep"), None),
            P("tp", ("grp", "rep"), None),
        ),
        check_vma=False,
    )
```

```python
import functools
import math

import jax
import jax.numpy as jnp
from jax import lax
from jax.experimental import pallas as pl
from jax.experimental.pallas import tpu as pltpu
from jax.sharding import PartitionSpec as P

HEADS = 16
KV_HEADS = 4
HEAD_DIM = 128
QBLOCK = 128


masked_low = -1e30
QUAD = 4
CHUNKS = 2


def gather_kernel(n_grp, own_ref, all_ref, local_sem, own_sems, z_send, z_recv, x_send, x_recv,
                  y_send, y_recv, d_send, d_recv, r_send, r_recv):
    g = lax.axis_index("grp")
    t = lax.axis_index("tp")
    r = lax.axis_index("rep")
    q = lax.rem(t, QUAD)
    qx = q + 1 - 2 * lax.rem(q, 2)
    qy = lax.rem(q + 2, QUAD)
    qd = lax.rem(qx + 2, QUAD)
    tx = t - q + qx
    ty = t - q + qy
    rows = own_ref.shape[0]
    size = rows // (QUAD * CHUNKS)
    others = n_grp - 1
    to_x, to_y, to_r = {"tp": tx}, {"tp": ty}, {"rep": 1 - r}
    mesh_ids = pl.DeviceIdType.MESH

    barrier = pltpu.get_barrier_semaphore()
    partners = [{"grp": lax.rem(g + k, n_grp)} for k in range(1, n_grp)] + [to_x, to_y, to_r]
    for partner in partners:
        pl.semaphore_signal(barrier, inc=1, device_id=partner, device_id_type=mesh_ids)
    pl.semaphore_wait(barrier, len(partners))

    def spot(quarter, c):
        return pl.ds(pl.multiple_of((quarter * CHUNKS + c) * size, size), size)

    def block(k):
        return lax.rem(g + k, n_grp) * 2 + r

    def sem_at(k, c):
        return c * others + k - 1

    def send(src, dst, sems, index, to):
        return pltpu.make_async_remote_copy(
            src_ref=src, dst_ref=dst, send_sem=sems[0].at[index], recv_sem=sems[1].at[index],
            device_id=to, device_id_type=mesh_ids)

    def forward(k, c, quarter, sems, index, to):
        part = all_ref.at[block(k), spot(quarter, c)]
        return send(part, part, sems, index, to)

    zs, xs, ys, ds, rs = ((z_send, z_recv), (x_send, x_recv), (y_send, y_recv),
                          (d_send, d_recv), (r_send, r_recv))
    started = []

    def go(copy):
        copy.start()
        started.append(copy)

    order = [1, n_grp - 1] + list(range(2, n_grp - 1)) if n_grp > 2 else [1]
    events = [(k, c) for c in range(CHUNKS) for k in order]
    for k, c in events:
        go(send(own_ref.at[spot(q, c)], all_ref.at[block(0), spot(q, c)], zs, sem_at(k, c),
                {"grp": lax.rem(g + n_grp - k, n_grp)}))
    local = pltpu.make_async_copy(own_ref, all_ref.at[block(0)], local_sem.at[0])
    local.start()
    own_swap = pltpu.make_async_remote_copy(
        src_ref=own_ref, dst_ref=all_ref.at[block(0)], send_sem=own_sems.at[0],
        recv_sem=own_sems.at[1], device_id=to_r, device_id_type=mesh_ids)
    own_swap.start()

    swaps = []

    def swap(k, c, quarter, lane):
        copy = forward(k, c, quarter, rs, lane * others * CHUNKS + sem_at(k, c), to_r)
        go(copy)
        swaps.append((k, c, (lane, sem_at(k, c))))

    def on_z(k, c):
        forward(k, c, q, zs, sem_at(k, c), to_x).wait_recv()
        go(forward(k, c, q, xs, sem_at(k, c), to_x))
        go(forward(k, c, q, ys, sem_at(k, c), to_y))
        swap(k, c, q, 0)

    def on_xy(k, c):
        forward(k, c, qx, xs, sem_at(k, c), to_x).wait_recv()
        if events.index((k, c)) % 2 == 0:
            go(forward(k, c, qx, ds, sem_at(k, c), to_y))
        swap(k, c, qx, 1)
        forward(k, c, qy, ys, sem_at(k, c), to_y).wait_recv()
        if events.index((k, c)) % 2 == 1:
            go(forward(k, c, qy, ds, sem_at(k, c), to_x))
        swap(k, c, qy, 2)

    def on_d(k, c):
        forward(k, c, qd, ds, sem_at(k, c), to_x).wait_recv()
        swap(k, c, qd, 3)

    lag = 2
    for i in range(len(events) + 2 * lag):
        if i < len(events):
            on_z(*events[i])
        if lag <= i < len(events) + lag:
            on_xy(*events[i - lag])
        if i >= 2 * lag:
            on_d(*events[i - 2 * lag])

    local.wait()
    own_swap.wait_send()
    for copy in started:
        copy.wait_send()
    peer = all_ref.at[lax.rem(g, n_grp) * 2 + 1 - r]
    pltpu.make_async_remote_copy(
        src_ref=own_ref, dst_ref=peer, send_sem=own_sems.at[0],
        recv_sem=own_sems.at[1], device_id=to_r, device_id_type=mesh_ids).wait_recv()
    for lane, quarter in enumerate((q, qx, qy, qd)):
        for k, c in events:
            part = all_ref.at[lax.rem(g + k, n_grp) * 2 + 1 - r, spot(quarter, c)]
            send(part, part, rs, lane * others * CHUNKS + sem_at(k, c), to_r).wait_recv()


def gather_columns(projection, n_grp, n_rep, n_tp):
    rows, width = projection.shape
    if n_rep != 2 or n_grp < 2 or n_tp % QUAD or rows % (QUAD * CHUNKS * 16):
        return lax.all_gather(projection, ("grp", "rep"), axis=0)
    steps = (n_grp - 1) * CHUNKS
    dma = pltpu.SemaphoreType.DMA
    total = n_grp * n_rep * rows * width
    return pl.pallas_call(
        functools.partial(gather_kernel, n_grp),
        out_shape=jax.ShapeDtypeStruct((n_grp * n_rep, rows, width), projection.dtype),
        in_specs=[pl.BlockSpec(memory_space=pltpu.VMEM)],
        out_specs=pl.BlockSpec(memory_space=pltpu.HBM),
        scratch_shapes=[dma((1,)), dma((2,))] + [dma((steps,))] * 8 + [dma((4 * steps,))] * 2,
        compiler_params=pltpu.CompilerParams(collective_id=0, has_side_effects=True),
        cost_estimate=pl.CostEstimate(flops=0, bytes_accessed=12 * total, transcendentals=0),
    )(projection)


NEAR = 4
SUBS = 4
SPARE = 2


def fused_kernel(n_grp, n_tp, q_in, k_in, v_in, codes_in, scales_in, proj_in, dq_ref, dk_ref, dv_ref,
                 q_v, k_all, v_all, codes_v, scales_ref, pq, stage, probs, wide, gathered, acc, errs, terms, sums,
                 pieces, peer_pieces, above, below, lsem, kvz_s, kvz_r, kvd_s, kvd_r, up_s, down_s, z_r,
                 pd_s, pd_r, zz_s, zz_r, zx_s, ag_s, ag_r, rs_s, rs_r, gd_s, gd_r, gz_s, gz_r):
    g = lax.axis_index("grp")
    t = lax.axis_index("tp")
    r = lax.axis_index("rep")
    rows = q_v.shape[0]
    head_dim = HEAD_DIM
    per = HEADS // KV_HEADS
    feats = per * head_dim
    slabs = codes_v.shape[0]
    width = codes_v.shape[2]
    half = proj_in.shape[1]
    steps = KV_HEADS * SUBS
    sub = proj_in.shape[0] // steps
    length = k_all.shape[0]
    inv_root = 1.0 / math.sqrt(head_dim)
    mesh_ids = pl.DeviceIdType.MESH
    other = {"rep": 1 - r}
    up = {"grp": jnp.minimum(g + 1, n_grp - 1)}
    down = {"grp": jnp.maximum(g - 1, 0)}
    has_up = g < n_grp - 1
    has_down = g > 0

    def peer_tp(m):
        return {"tp": lax.rem(t + m, n_tp)}

    def sender(m):
        return lax.rem(t + n_tp - m, n_tp)

    def send(src, dst, send_sem, recv_sem, to):
        return pltpu.make_async_remote_copy(src_ref=src, dst_ref=dst, send_sem=send_sem, recv_sem=recv_sem,
                                            device_id=to, device_id_type=mesh_ids)

    def arrived(dst, send_sem, recv_sem):
        send(dst, dst, send_sem, recv_sem, other).wait_recv()

    ended = []

    def go(copy, when=None):
        if when is None:
            copy.start()
        else:
            pl.when(when)(copy.start)
        ended.append((copy, when))

    def block(s, core):
        return pl.ds(pl.multiple_of((s * 2 + core) * rows, rows), rows)

    def local(src, dst, index):
        copy = pltpu.make_async_copy(src, dst, lsem.at[index])
        copy.start()
        return copy

    own_k = local(k_in.at[0], k_all.at[block(g, r)], 0)
    own_v = local(v_in.at[0], v_all.at[block(g, r)], 1)
    own_q = local(q_in.at[0], q_v, 2)
    own_codes = local(codes_in, codes_v, 3)
    own_scales = local(scales_in, scales_ref, 4)
    own_cols = pltpu.make_async_copy(proj_in, pq.at[r], lsem.at[5])
    mine = t == g
    pl.when(mine)(own_cols.start)

    barrier = pltpu.get_barrier_semaphore()
    greeted = [other] + [peer_tp(m) for m in range(1, n_tp)] + [{"grp": lax.rem(g + m, n_grp)} for m in range(1, n_grp)]
    for to in greeted:
        pl.semaphore_signal(barrier, inc=1, device_id=to, device_id_type=mesh_ids)
    pl.semaphore_wait(barrier, len(greeted))

    kv = ((k_in, k_all), (v_in, v_all))
    for i, (src, dst) in enumerate(kv):
        go(send(src.at[0], dst.at[block(g, r)], kvz_s.at[i, g], kvz_r.at[i, g], up), has_up)
    for i, (src, dst) in enumerate(kv):
        go(send(src.at[0], dst.at[block(g, r)], kvd_s.at[i, g], kvd_r.at[i, g], other))

    def span(k):
        return pl.ds(k * sub if isinstance(k, int) else pl.multiple_of(k * sub, sub), sub)

    def placed(core, k):
        return pq.at[core, span(k)]

    def own_down(k):
        return send(proj_in.at[span(k)], placed(r, k), down_s.at[k], z_r.at[k], down)

    def own_up(k):
        return send(proj_in.at[span(k)], placed(r, k), up_s.at[k], z_r.at[k], up)

    def own_over(k):
        return send(proj_in.at[span(k)], placed(r, k), pd_s.at[k], pd_r.at[k], other)

    for k in range(steps):
        go(own_down(k), jnp.logical_and(mine, has_down))
    for k in range(steps):
        go(own_over(k), mine)

    for s in range(1, n_grp):
        @pl.when(s > g)
        def _():
            unseen = pl.ds(s * 2 * rows, 2 * rows)
            k_all[unseen] = jnp.zeros((2 * rows, k_all.shape[1]), k_all.dtype)
            v_all[unseen] = jnp.zeros((2 * rows, v_all.shape[1]), v_all.dtype)

    own_codes.wait()
    own_scales.wait()
    scales = [scales_ref[u].astype(jnp.float32).T for u in range(slabs)]
    for b in range(width // QBLOCK):
        at = pl.ds(b * QBLOCK, QBLOCK)
        for u in range(slabs):
            acc[u * rows:(u + 1) * rows, at] = -(codes_v[u, :, at].astype(jnp.float32) * scales[u][:, b:b + 1])

    for d in range(1, n_grp):
        s = jnp.maximum(g - d, 0)
        here = g >= d
        for i, (_, dst) in enumerate(kv):
            part = dst.at[block(s, r)]
            pl.when(here)(functools.partial(arrived, part, kvz_s.at[i, s], kvz_r.at[i, s]))
            go(send(part, part, kvz_s.at[i, s], kvz_r.at[i, s], up), jnp.logical_and(here, has_up))
            go(send(part, part, kvd_s.at[i, s], kvd_r.at[i, s], other), here)

    direct = steps - SPARE
    idle = t == n_tp - 1

    def spare_up(s, a, own=False):
        src = proj_in.at[span(direct + a)] if own else stage.at[s, a]
        return send(src, stage.at[s, a], zz_s.at[s, a], zz_r.at[s, a], up)

    def spare_out(s, a):
        return send(stage.at[s, a], placed(r, direct + a), zx_s.at[s, a], z_r.at[direct + a], {"tp": s})

    for k in range(direct):
        go(own_up(k), jnp.logical_and(mine, has_up))
    for s in range(n_grp - 1):
        for a in range(SPARE):
            go(spare_up(s, a, own=True), jnp.logical_and(idle, g == s))

    def spare_in(act, wait):
        for s in range(n_grp - 2, -1, -1):
            for a in range(SPARE):
                @pl.when(jnp.logical_and(idle, g > s))
                def _(s=s, a=a):
                    if wait:
                        arrived(stage.at[s, a], zz_s.at[s, a], zz_r.at[s, a])
                    pl.when(has_up)(lambda: act(spare_up(s, a)))
                    act(spare_out(s, a))

    def begin(copy):
        copy.start()

    pl.when(g == 1)(lambda: spare_in(begin, True))

    own_k.wait()
    own_v.wait()
    own_q.wait()
    for s in range(n_grp):
        for i, (_, dst) in enumerate(kv):
            part = dst.at[block(s, 1 - r)]
            pl.when(s <= g)(functools.partial(arrived, part, kvd_s.at[i, s], kvd_r.at[i, s]))

    first = (g * 2 + r) * rows
    row_pos = first + lax.rem(lax.broadcasted_iota(jnp.int32, (per * rows, length), 0), rows)
    allowed = lax.broadcasted_iota(jnp.int32, (per * rows, length), 1) <= row_pos

    def head_cols(kh, j=0):
        return pl.ds(pl.multiple_of(kh * feats + j * head_dim, head_dim), head_dim)

    def kv_cols(kh):
        return pl.ds(pl.multiple_of(kh * head_dim, head_dim), head_dim)

    def stacked_queries(kh):
        return jnp.concatenate([q_v[:, head_cols(kh, j)] for j in range(per)], axis=0)

    def ag_copy(kh, m):
        part = gathered.at[t, kh]
        return send(part, part, ag_s.at[m - 1, kh], ag_r.at[m - 1, kh], peer_tp(m))

    rising = t < g
    falling = t > g
    onward_up = jnp.logical_and(rising, has_up)
    onward_down = jnp.logical_and(falling, has_down)
    onward = jnp.logical_or(onward_up, onward_down)
    foreign = t != g

    def relay_up(k):
        return send(placed(r, k), placed(r, k), up_s.at[k], z_r.at[k], up)

    def relay_down(k):
        return send(placed(r, k), placed(r, k), down_s.at[k], z_r.at[k], down)

    def relay_over(k):
        return send(placed(r, k), placed(r, k), pd_s.at[k], pd_r.at[k], other)

    def receive_one(k):
        arrived(placed(r, k), up_s.at[k], z_r.at[k])
        pl.when(jnp.logical_and(onward_up, k < direct))(lambda: relay_up(k).start())
        pl.when(onward_down)(lambda: relay_down(k).start())
        relay_over(k).start()

    def receive(kh):
        for i in range(SUBS):
            receive_one(kh * SUBS + i)

    def forward(kh, carry):
        pl.when(onward)(lambda: receive_one(kh))
        scores = lax.dot_general(stacked_queries(kh), k_all[:, kv_cols(kh)], (((1,), (1,)), ((), ())),
                                 preferred_element_type=jnp.float32) * inv_root
        scores = jnp.where(allowed, scores, masked_low)
        shifted = jnp.exp(scores - scores.max(-1, keepdims=True))
        low = (shifted / shifted.sum(-1, keepdims=True)).astype(jnp.bfloat16)
        probs[kh] = low
        out = jnp.dot(low, v_all[:, kv_cols(kh)], preferred_element_type=jnp.float32)
        wide[kh] = out
        out_low = out.astype(jnp.bfloat16)
        for j in range(per):
            gathered[t, kh, :, j * head_dim:(j + 1) * head_dim] = out_low[j * rows:(j + 1) * rows]
        for m in range(1, n_tp):
            ag_copy(kh, m).start()
        return carry

    lax.fori_loop(0, KV_HEADS, forward, 0)

    def proj_rows(kh):
        return pl.ds(pl.multiple_of(kh * feats, feats), feats)

    def project(kh):
        for m in range(1, n_tp):
            arrived(gathered.at[sender(m), kh], ag_s.at[m - 1, kh], ag_r.at[m - 1, kh])
        for i in range(SUBS):
            k = kh * SUBS + i
            arrived(placed(1 - r, k), pd_s.at[k], pd_r.at[k])
        left = jnp.concatenate([gathered[u, kh] for u in range(slabs)], axis=0)
        for b in range(2):
            acc[:, b * half:(b + 1) * half] += jnp.dot(left, pq[b, proj_rows(kh)],
                                                       preferred_element_type=jnp.float32)

    pl.when(mine)(own_cols.wait)
    behind = jnp.where(onward, KV_HEADS, 0)

    def collect(i, carry):
        pl.when(jnp.logical_and(jnp.logical_and(foreign, i < KV_HEADS), jnp.logical_or(i > 0, jnp.logical_not(onward))))(lambda: receive(i))
        pl.when(jnp.logical_and(g > 1, i == jnp.where(onward, 1, 0)))(lambda: spare_in(begin, True))
        pl.when(i >= behind)(lambda: project(i - behind))
        return carry

    lax.fori_loop(0, KV_HEADS + behind, collect, 0)
    errs[...] = acc[...].astype(jnp.bfloat16)

    def rs_copy(kh, m):
        return send(terms.at[kh, lax.rem(t + m, n_tp)], sums.at[kh, m - 1], rs_s.at[m - 1, kh],
                    rs_r.at[m - 1, kh], peer_tp(m))

    def back_project(kh, carry):
        total = jnp.zeros((slabs * rows, feats), jnp.float32)
        for b in range(2):
            total += lax.dot_general(errs[:, b * half:(b + 1) * half], pq[b, proj_rows(kh)],
                                     (((1,), (1,)), ((), ())), preferred_element_type=jnp.float32)
        for u in range(slabs):
            terms[kh, u] = total[u * rows:(u + 1) * rows].astype(jnp.bfloat16)
        for m in range(1, n_tp):
            rs_copy(kh, m).start()
        return carry

    lax.fori_loop(0, KV_HEADS, back_project, 0)

    def gd_copy(kh):
        return send(pieces.at[kh, 1 - r], peer_pieces.at[kh], gd_s.at[kh], gd_r.at[kh], other)

    def backward(kh):
        grad = terms[kh, t].astype(jnp.float32)
        for m in range(1, n_tp):
            arrived(sums.at[kh, m - 1], rs_s.at[m - 1, kh], rs_r.at[m - 1, kh])
            grad += sums[kh, m - 1].astype(jnp.float32)
        grad = grad.astype(jnp.bfloat16)
        grad = jnp.concatenate([grad[:, j * head_dim:(j + 1) * head_dim] for j in range(per)], axis=0)
        delta = (grad.astype(jnp.float32) * wide[kh]).sum(-1, keepdims=True)
        low = probs[kh]
        grad_prob = lax.dot_general(grad, v_all[:, kv_cols(kh)], (((1,), (1,)), ((), ())),
                                    preferred_element_type=jnp.float32)
        score = (low.astype(jnp.float32) * (grad_prob - delta) * inv_root).astype(jnp.bfloat16)
        dq = jnp.dot(score, k_all[:, kv_cols(kh)], preferred_element_type=jnp.float32).astype(jnp.bfloat16)
        for j in range(per):
            dq_ref[0, :, head_cols(kh, j)] = dq[j * rows:(j + 1) * rows]
        over_rows = (((0,), (0,)), ((), ()))
        for i, (lhs, rhs) in enumerate(((stacked_queries(kh), score), (grad, low))):
            term = lax.dot_general(lhs, rhs, over_rows, preferred_element_type=jnp.float32).astype(jnp.bfloat16)
            for s in range(n_grp):
                for core in range(2):
                    at = (s * 2 + core) * rows
                    pieces[kh, core, s, i * head_dim:(i + 1) * head_dim, :] = term[:, at:at + rows]
        gd_copy(kh).start()

    def gz_copy(kh, s):
        return send(below.at[kh, s], above.at[kh, g], gz_s.at[kh, s], gz_r.at[kh, g], {"grp": s})

    def both_cores(kh, s):
        return pieces[kh, r, s].astype(jnp.float32) + peer_pieces[kh, s].astype(jnp.float32)

    def hand_down(kh):
        arrived(peer_pieces.at[kh], gd_s.at[kh], gd_r.at[kh])
        for s in range(n_grp - 1):
            @pl.when(s < g)
            def _():
                below[kh, s] = both_cores(kh, s).astype(jnp.bfloat16)
                gz_copy(kh, s).start()

    def settle(kh):
        wide_sum[...] = both_cores(kh, g)
        for s in range(1, n_grp):
            @pl.when(s > g)
            def _():
                arrived(above.at[kh, s], gz_s.at[kh, s], gz_r.at[kh, s])
                wide_sum[...] += above[kh, s].astype(jnp.float32)
        done = wide_sum[...]
        dk_ref[0, :, kv_cols(kh)] = done[:head_dim].T.astype(jnp.bfloat16)
        dv_ref[0, :, kv_cols(kh)] = done[head_dim:].T.astype(jnp.bfloat16)

    def last(kh, carry):
        backward(kh)
        hand_down(kh)
        return carry

    def finish(kh, carry):
        settle(kh)
        return carry

    wide_sum = acc.at[pl.ds(0, 2 * head_dim), pl.ds(0, rows)]
    lax.fori_loop(0, KV_HEADS, last, 0)
    lax.fori_loop(0, KV_HEADS, finish, 0)

    for copy, when in ended:
        if when is None:
            copy.wait_send()
        else:
            pl.when(when)(copy.wait_send)

    spare_in(lambda copy: copy.wait_send(), False)

    def relayed(k, carry):
        relay_over(k).wait_send()
        pl.when(jnp.logical_and(onward_up, k < direct))(lambda: relay_up(k).wait_send())
        pl.when(onward_down)(lambda: relay_down(k).wait_send())
        return carry

    pl.when(foreign)(lambda: lax.fori_loop(0, steps, relayed, None))

    def sent(kh, carry):
        for m in range(1, n_tp):
            ag_copy(kh, m).wait_send()
            rs_copy(kh, m).wait_send()
        gd_copy(kh).wait_send()
        for s in range(n_grp - 1):
            pl.when(s < g)(lambda s=s: gz_copy(kh, s).wait_send())
        return carry

    lax.fori_loop(0, KV_HEADS, sent, 0)


def hand_out(dq_in, dk_in, dv_in, dq_out, dk_out, dv_out, sems):
    pairs = ((dq_in, dq_out), (dk_in, dk_out), (dv_in, dv_out))
    copies = [pltpu.make_async_copy(src, dst, sems.at[i]) for i, (src, dst) in enumerate(pairs)]
    for copy in copies:
        copy.start()
    for copy in copies:
        copy.wait()


def fused(mesh, query_rows, key_rows, value_rows, teacher_codes, teacher_scales, projection):
    n_grp, n_tp = mesh.shape["grp"], mesh.shape["tp"]
    rows, depth = query_rows.shape[1:]
    kv_width = key_rows.shape[2]
    slabs, _, width = teacher_codes.shape
    half = projection.shape[1]
    length = n_grp * 2 * rows
    per = HEADS // KV_HEADS
    feats = per * HEAD_DIM
    steps = KV_HEADS * SUBS
    low, wide = jnp.bfloat16, jnp.float32
    vmem = pltpu.VMEM
    dma = pltpu.SemaphoreType.DMA
    hbm_spec = pl.BlockSpec(memory_space=pltpu.HBM)
    flat_scales = teacher_scales.transpose(0, 2, 1)
    vmem_spec = pl.BlockSpec(memory_space=pltpu.VMEM)
    scratch = [
        vmem((rows, depth), low), vmem((length, kv_width), low), vmem((length, kv_width), low),
        vmem((slabs, rows, width), low), vmem(flat_scales.shape, low), vmem((2, depth, half), low),
        vmem((n_grp - 1, SPARE, depth // steps, half), low),
        vmem((KV_HEADS, per * rows, length), low), vmem((KV_HEADS, per * rows, HEAD_DIM), wide),
        vmem((slabs, KV_HEADS, rows, feats), low), vmem((slabs * rows, width), wide),
        vmem((slabs * rows, width), low), vmem((KV_HEADS, slabs, rows, feats), low),
        vmem((KV_HEADS, n_tp - 1, rows, feats), low), vmem((KV_HEADS, 2, n_grp, 2 * HEAD_DIM, rows), low),
        vmem((KV_HEADS, n_grp, 2 * HEAD_DIM, rows), low), vmem((KV_HEADS, n_grp, 2 * HEAD_DIM, rows), low),
        vmem((KV_HEADS, n_grp, 2 * HEAD_DIM, rows), low),
        dma((6,)), dma((2, n_grp)), dma((2, n_grp)), dma((2, n_grp)), dma((2, n_grp)),
        dma((steps,)), dma((steps,)), dma((steps,)), dma((steps,)), dma((steps,)),
        dma((n_grp - 1, SPARE)), dma((n_grp - 1, SPARE)), dma((n_grp - 1, SPARE)),
        dma((n_tp - 1, KV_HEADS)), dma((n_tp - 1, KV_HEADS)), dma((n_tp - 1, KV_HEADS)),
        dma((n_tp - 1, KV_HEADS)), dma((KV_HEADS,)), dma((KV_HEADS,)),
        dma((KV_HEADS, n_grp)), dma((KV_HEADS, n_grp)),
    ]
    outs = [jax.ShapeDtypeStruct(a.shape, a.dtype) for a in (query_rows, key_rows, value_rows)]
    grads = pl.pallas_call(
        functools.partial(fused_kernel, n_grp, n_tp),
        out_shape=outs,
        in_specs=[hbm_spec] * 6,
        out_specs=[vmem_spec] * 3,
        scratch_shapes=scratch,
        compiler_params=pltpu.CompilerParams(collective_id=1, has_side_effects=True,
                                             vmem_limit_bytes=60 * 2 ** 20),
    )(query_rows, key_rows, value_rows, teacher_codes, flat_scales, projection)
    return pl.pallas_call(
        hand_out,
        out_shape=outs,
        in_specs=[pl.BlockSpec(memory_space=pl.ANY)] * 3,
        out_specs=[hbm_spec] * 3,
        scratch_shapes=[dma((len(outs),))],
        compiler_params=pltpu.CompilerParams(vmem_limit_bytes=2 ** 20),
    )(*grads)


def suits(mesh, teacher_codes, projection):
    depth, half = projection.shape
    n_grp, n_tp, n_rep = (mesh.shape[axis] for axis in ("grp", "tp", "rep"))
    return (n_rep == 2 and 1 < n_grp == n_tp <= NEAR and teacher_codes.shape[2] == 2 * half
            and depth % (KV_HEADS * SUBS * 16) == 0)


def shards(mesh, query_rows, key_rows, value_rows, teacher_codes, teacher_scales, projection):
    if suits(mesh, teacher_codes, projection):
        return tuple(fused(mesh, query_rows, key_rows, value_rows, teacher_codes, teacher_scales, projection))
    rows_dev = query_rows.shape[1]
    group_size = HEADS // KV_HEADS
    inv_root = 1.0 / math.sqrt(HEAD_DIM)
    kv_width = key_rows.shape[2]
    pairs_all = lax.all_gather(
        jnp.concatenate([key_rows, value_rows], 2), ("grp", "rep"), axis=1, tiled=True
    )
    keys_all, values_all = pairs_all[..., :kv_width], pairs_all[..., kv_width:]
    length = keys_all.shape[1]
    my_index = lax.axis_index(("grp", "rep"))
    first_row = my_index * rows_dev
    queries = query_rows[0].reshape(rows_dev, KV_HEADS, group_size, HEAD_DIM).transpose(1, 2, 0, 3)
    key_heads = keys_all[0].reshape(length, KV_HEADS, HEAD_DIM).transpose(1, 0, 2)
    value_heads = values_all[0].reshape(length, KV_HEADS, HEAD_DIM).transpose(1, 0, 2)
    row_pos = first_row + jnp.arange(rows_dev, dtype=jnp.int32)
    slab_codes, slab_scales = (
        lax.all_to_all(teacher_codes, "tp", split_axis=0, concat_axis=2, tiled=True),
        lax.all_to_all(teacher_scales, "tp", split_axis=0, concat_axis=2, tiled=True),
    )

    raw_scores = (
        jnp.einsum("hgqd,hkd->hgqk", queries, key_heads, preferred_element_type=jnp.float32)
        * inv_root
    )
    allowed = jnp.arange(length, dtype=jnp.int32)[None, :] <= row_pos[:, None]
    scores = jnp.where(allowed, raw_scores, masked_low)
    row_peak = scores.max(-1, keepdims=True)
    shifted = jnp.exp(scores - row_peak)
    probs = shifted / shifted.sum(-1, keepdims=True)
    prob_low = probs.astype(jnp.bfloat16)
    attn_wide = jnp.einsum(
        "hgqk,hkd->hgqd", prob_low, value_heads, preferred_element_type=jnp.float32
    )
    attn_low = (
        attn_wide.transpose(2, 0, 1, 3).reshape(rows_dev, HEADS * HEAD_DIM).astype(jnp.bfloat16)
    )
    col_width = projection.shape[1]
    shaped = gather_columns(
        projection, mesh.shape["grp"], mesh.shape["rep"], mesh.shape["tp"]
    )
    pieces = shaped.shape[0]
    approx = jnp.einsum("td,sdc->tsc", attn_low, shaped, preferred_element_type=jnp.float32)
    code_rows = slab_codes[0].astype(jnp.float32)
    scale_rows = slab_scales[0].astype(jnp.float32)
    target = (code_rows.reshape(rows_dev, -1, QBLOCK) * scale_rows[..., None]).reshape(
        rows_dev, pieces, col_width
    )
    errors = (approx - target).astype(jnp.bfloat16)
    partial_terms = jnp.einsum(
        "tsc,sdc->std", errors, shaped, preferred_element_type=jnp.float32
    ).astype(jnp.bfloat16)
    grad_attn = partial_terms.astype(jnp.float32).sum(0)
    grad_low = grad_attn.astype(jnp.bfloat16)
    grad_heads = grad_low.reshape(rows_dev, KV_HEADS, group_size, HEAD_DIM).transpose(1, 2, 0, 3)
    row_delta = (grad_heads.astype(jnp.float32) * attn_wide).sum(-1)

    grad_values = jnp.einsum(
        "hgqk,hgqd->hkd", prob_low, grad_heads, preferred_element_type=jnp.float32
    )
    grad_prob = jnp.einsum(
        "hgqd,hkd->hgqk", grad_heads, value_heads, preferred_element_type=jnp.float32
    )
    grad_score = (probs * (grad_prob - row_delta[..., None]) * inv_root).astype(jnp.bfloat16)
    grad_queries = jnp.einsum(
        "hgqk,hkd->hgqd", grad_score, key_heads, preferred_element_type=jnp.float32
    )
    grad_keys = jnp.einsum(
        "hgqk,hgqd->hkd", grad_score, queries, preferred_element_type=jnp.float32
    )
    key_terms = grad_keys.transpose(1, 0, 2).reshape(1, length, KV_HEADS * HEAD_DIM)
    value_terms = grad_values.transpose(1, 0, 2).reshape(1, length, KV_HEADS * HEAD_DIM)
    pair_terms = jnp.concatenate([key_terms, value_terms], 2).astype(jnp.bfloat16)
    pair_grad = lax.psum_scatter(
        pair_terms, ("grp", "rep"), scatter_dimension=1, tiled=True
    )
    key_grad, value_grad = pair_grad[..., :kv_width], pair_grad[..., kv_width:]
    query_grad = (
        grad_queries.transpose(2, 0, 1, 3)
        .reshape(1, rows_dev, HEADS * HEAD_DIM)
        .astype(jnp.bfloat16)
    )
    return (query_grad, key_grad.astype(jnp.bfloat16), value_grad.astype(jnp.bfloat16))


def solution(mesh):
    placed = (
        P("tp", ("grp", "rep"), None),
        P("tp", ("grp", "rep"), None),
        P("tp", ("grp", "rep"), None),
        P(None, ("grp", "rep"), "tp"),
        P(None, ("grp", "rep"), "tp"),
        P(None, ("grp", "rep")),
    )
    return jax.shard_map(
        functools.partial(shards, mesh),
        mesh=mesh,
        in_specs=placed,
        out_specs=(
            P("tp", ("grp", "rep"), None),
            P("tp", ("grp", "rep"), None),
            P("tp", ("grp", "rep"), None),
        ),
        check_vma=False,
    )
```
